32 devices in a mesh: row: 8 (over z, x), col: 4 (over y, core).
Axes of the slice: x: 2, y: 2, z: 4, core: 2. Of those that a mesh axis runs over, the one named last changes fastest.
Arguments:
- matrix: float32 [5, 8, 10, 4, 128, 128], P(None, 'row', None, 'col'), may hold values from 0 to 2.5, as said below
- flags: int32 [5, 8, 10, 4], P(None, 'row', None, 'col'), may hold values from 0 to 1, as said below
Outputs:
- factor: float32 [5, 8, 10, 4, 128, 128], P(None, 'row', None, 'col')
The draws below stay inside these ranges and needn't reach their ends.
Inputs may be any that keep to these rules, and one draw needn't show every extreme that they name: `matrix`: symmetric positive definite, of order 40*128, diagonal at least 1.5. `flags`: 0 marks a float32 tile, 1 a bfloat16 tile; every diagonal tile is 0.
All inputs are finite; a program needn't handle non-finite values.
Results may differ from the reference program's by a relative error of at most 0.0005.
The reference program's roundings to bfloat16 on the way count: a program that leaves them out, or rounds other values in their place, can miss the bound.
Values sent between devices are 32-bit elements; how exact they have to be, the bound alone decides.
A program may use at most 128 MiB of HBM per device.

```python
import jax
import jax.numpy as jnp
from jax import lax

B = 128
PT = 4
TR_DEV = 5
NT = 40
TC_DEV = 10


def draw_matrix(key, part):
    count = NT * B
    points = jax.random.uniform(jax.random.fold_in(key, 11), (count, 2), jnp.float32)
    order = jnp.argsort(points[:, 0])
    points = points[order]
    reach = 0.6
    nugget = 0.5
    delta_x = points[:, 0][:, None] - points[:, 0][None, :]
    delta_y = points[:, 1][:, None] - points[:, 1][None, :]
    dist = jnp.sqrt(delta_x * delta_x + delta_y * delta_y)
    cov = jnp.exp(-dist / reach) + nugget * jnp.eye(count, dtype=jnp.float32)
    tiled = cov.reshape(NT, B, NT, B).transpose(0, 2, 1, 3)
    return tiled.reshape(TR_DEV, NT // TR_DEV, TC_DEV, NT // TC_DEV, B, B)


def draw_flags(key, part):
    tile_ids = jnp.arange(NT, dtype=jnp.int32)
    spacing = jnp.abs(tile_ids[:, None] - tile_ids[None, :])
    band = jax.random.randint(jax.random.fold_in(key, 5), (), 2, 6)
    flips = jax.random.randint(jax.random.fold_in(key, 7), (NT, NT), 0, 4)
    far_mark = (flips != 0).astype(jnp.int32)
    near_mark = (flips == 0).astype(jnp.int32)
    marks = jnp.where(spacing == 0, 0, jnp.where(spacing >= band, far_mark, near_mark))
    return marks.astype(jnp.int32).reshape(TR_DEV, NT // TR_DEV, TC_DEV, NT // TC_DEV)


def setup_inputs(seed: int = 0) -> dict:
    key_list = jax.random.split(jax.random.key(seed), 3)
    matrix = draw_matrix(jax.random.fold_in(key_list[2], 71), 0)
    flags = draw_flags(jax.random.fold_in(key_list[2], 71), 0)
    return {"matrix": matrix, "flags": flags}


def storage_round(values):
    narrow = lax.optimization_barrier(values.astype(jnp.bfloat16))
    return narrow.astype(jnp.float32)

def reference(matrix, flags):
    width = PT * B
    tiles = matrix.reshape(NT, NT, B, B)
    marks = flags.reshape(NT, NT)
    work = jnp.where((marks == 1)[:, :, None, None], storage_round(tiles), tiles)
    tile_ids = jnp.arange(NT, dtype=jnp.int32)
    for step in range(2):
        start = step * PT
        rows = work[:, start:start + PT].transpose(0, 2, 1, 3).reshape(NT, B, width)
        dense = rows[start:start + PT].reshape(width, width)
        sym = jnp.tril(dense) + jnp.tril(dense, -1).T
        lower_block = jnp.linalg.cholesky(sym)
        flat = rows.reshape(NT * B, width)
        solved = jax.scipy.linalg.solve_triangular(lower_block, flat.T, lower=True).T.reshape(NT, B, width)
        solved = solved.at[start:start + PT].set(lower_block.reshape(PT, B, width))
        rounded = storage_round(solved)

        def row_update(args):
            tile_row, mark_row, index = args
            exact = jnp.einsum('ik,cjk->cij', solved[index], solved, precision=lax.Precision.HIGHEST)
            coarse = jnp.einsum('ik,cjk->cij', rounded[index], rounded, precision=lax.Precision.HIGHEST)
            live = (index >= tile_ids) & (tile_ids >= start + PT)
            updated = jnp.where((mark_row == 1)[:, None, None], tile_row - coarse, tile_row - exact)
            return jnp.where(live[:, None, None], updated, tile_row)
        work = lax.map(row_update, (work, marks, tile_ids))
        new_cols = solved.reshape(NT, B, PT, B).transpose(0, 2, 1, 3)
        keep = (tile_ids >= start)[:, None, None, None]
        work = work.at[:, start:start + PT].set(jnp.where(keep, new_cols, work[:, start:start + PT]))
    final = jnp.where((marks == 1)[:, :, None, None], storage_round(work), work)
    upper = tile_ids[:, None] < tile_ids[None, :]
    final = jnp.where(upper[:, :, None, None], jnp.float32(0.0), final)
    return final.reshape(TR_DEV, NT // TR_DEV, TC_DEV, NT // TC_DEV, B, B)
```

```python
import jax
import jax.numpy as jnp
from jax import lax
from jax.experimental import pallas as pl
from jax.experimental.pallas import tpu as pltpu
from jax.sharding import PartitionSpec as P

PT = 4
MICRO = 16
NT_DIMS = (((1,), (1,)), ((), ()))
TN_DIMS = (((0,), (0,)), ((), ()))


def dot_nt(a, b):
    return lax.dot_general(
        a, b, NT_DIMS, precision=lax.Precision.HIGHEST, preferred_element_type=jnp.float32
    )


def dot_nt_coarse(a, b):
    return lax.dot_general(
        a.astype(jnp.bfloat16),
        b.astype(jnp.bfloat16),
        NT_DIMS,
        preferred_element_type=jnp.float32,
    )


def split(value):
    high = value.astype(jnp.bfloat16)
    return high, (value - high.astype(jnp.float32)).astype(jnp.bfloat16)


def dot_bf16(a, b):
    return lax.dot_general(a, b, NT_DIMS, preferred_element_type=jnp.float32)


def dot_pairs(a, b):
    return dot_bf16(a[0], b[0]) + (dot_bf16(a[0], b[1]) + dot_bf16(a[1], b[0]))


def factor_tile(start, work_ref, low_ref, inv_ref):
    tile = start.shape[0]
    lane = lax.broadcasted_iota(jnp.int32, (tile, tile), 1)
    sub = lax.broadcasted_iota(jnp.int32, (tile, tile), 0)
    work_ref[:, :tile] = start
    work_ref[:, tile:] = (lane == sub).astype(jnp.float32)
    lane8 = lax.broadcasted_iota(jnp.int32, (MICRO, tile), 1)
    sub8 = lax.broadcasted_iota(jnp.int32, (MICRO, tile), 0)

    def micro(p, carry):
        base = pl.multiple_of(p * MICRO, MICRO)
        both = work_ref[pl.ds(base, MICRO), :]
        turned = pltpu.roll(both[:, :tile], lax.rem(tile - base, tile), 1)
        s = {}
        for k in range(MICRO):
            for q in range(k + 1):
                s[k, q] = jnp.broadcast_to(turned[k : k + 1, q : q + 1], (1, tile))
        rows = [both[k : k + 1, :tile] for k in range(MICRO)]
        more = [both[k : k + 1, tile:] for k in range(MICRO)]
        for q in range(MICRO):
            d = s[q, q]
            r = lax.rsqrt(d)
            r = r * (1.5 - 0.5 * d * r * r)
            rows[q] = rows[q] * r
            more[q] = more[q] * r
            low = {k: s[k, q] * r for k in range(q + 1, MICRO)}
            for k in range(q + 1, MICRO):
                for m in range(q + 1, k + 1):
                    s[k, m] = s[k, m] - low[k] * low[m]
                rows[k] = rows[k] - low[k] * rows[q]
                more[k] = more[k] - low[k] * more[q]
        upper = jnp.where(lane8 >= base + sub8, jnp.concatenate(rows, axis=0), 0.0)
        extra = jnp.concatenate(more, axis=0)
        low_ref[pl.ds(base, MICRO), :] = upper
        inv_ref[pl.ds(base, MICRO), :] = extra
        work_ref[...] -= lax.dot_general(
            upper,
            jnp.concatenate([upper, extra], axis=1),
            TN_DIMS,
            precision=lax.Precision.HIGHEST,
            preferred_element_type=jnp.float32,
        )
        return carry

    lax.fori_loop(0, tile // MICRO, micro, 0)


def exchange_kernel(dims, p_ref, own_ref, across_ref, low0_ref, inv0_ref, low1_ref, inv1_ref,
                    grid_ref, relay_ref, work_ref, up_ref,
                    line_send, line_recv, spread_send, grid_recv, own_send, own_recv,
                    column_send, across_recv, cross_send, result_send, result_recv, local_sem):
    rows, cols, slots, skip, tile = dims
    count = 2 * PT
    groups = rows // cols
    lines = rows // 2
    row = lax.axis_index("row")
    col = lax.axis_index("col")
    along, side = row // 2, row % 2
    wide, core = col // 2, col % 2
    relays = (row + col) % 2 == 0
    works = (row + col) % 2 == 1
    partner = wide * 2 + 1 - core
    bulk = p_ref.at[skip:]

    def copy(src, dst, send, recv, to_row, to_col):
        return pltpu.make_async_remote_copy(
            src_ref=src, dst_ref=dst, send_sem=send, recv_sem=recv,
            device_id=(to_row, to_col), device_id_type=pl.DeviceIdType.MESH,
        )

    def line_copies(act):
        for s in range(slots):
            for k in range(lines):
                here = (k == along) & (core == side)

                @pl.when((s * cols + col <= row) & (row < count) & jnp.logical_not(here))
                def _():
                    act(copy(p_ref.at[0, s], relay_ref.at[along, core, s], line_send.at[s, k],
                             line_recv.at[along, core, s], 2 * k + side, wide * 2 + side))

    def spread_copies(first, last, act, wait):
        for k in range(first // 2, last // 2):
            for c in range(2):
                for s in range(slots):
                    mine = (k == along) & (core == c)
                    from_col = wide * 2 + c
                    from_row = 2 * k + side
                    need = s * cols + from_col <= from_row

                    def targets(src):
                        for n in range(2):
                            for w in range(cols // 2):
                                act(copy(src, grid_ref.at[from_row, from_col, s],
                                         spread_send.at[k, c, s, n, w],
                                         grid_recv.at[from_row, from_col, s],
                                         2 * along + n, 2 * w + 1 - n))

                    @pl.when(need & mine)
                    def _():
                        targets(p_ref.at[0, s])

                    @pl.when(need & jnp.logical_not(mine))
                    def _():
                        if wait:
                            copy(p_ref.at[0, s], relay_ref.at[k, c, s], line_send.at[s, 0],
                                 line_recv.at[k, c, s], row, partner).wait_recv()
                        targets(relay_ref.at[k, c, s])

    def own_copies(act):
        for k in range(1, cols):
            act(copy(bulk, own_ref.at[col], own_send.at[k], own_recv.at[col], row, (col + k) % cols))

    def column_copies(act):
        for k in range(lines):
            @pl.when(jnp.logical_not((k == along) & (col == row % cols)))
            def _():
                act(copy(bulk, across_ref.at[row // cols, col], column_send.at[k],
                         across_recv.at[row // cols, col], 2 * k + side, row % cols))

    def cross(act, wait):
        near = jnp.clip((along - wide + cols // 4) // (cols // 2), 0, groups - 1)
        for k in range(cols):
            from_col = (wide + k // 2) % (cols // 2) * 2 + (core + k) % 2
            for h in range(groups):
                g = (near + h) % groups
                mine = (g * cols + col == row) & (from_col == col)

                def forward(src):
                    return copy(src, across_ref.at[g, from_col], cross_send.at[g, from_col],
                                across_recv.at[g, from_col], 2 * along + 1 - side, col)

                @pl.when(mine)
                def _():
                    act(forward(bulk))

                @pl.when(jnp.logical_not(mine))
                def _():
                    move = forward(across_ref.at[g, from_col])
                    if wait:
                        move.wait_recv()
                    act(move)

    def wait_grid(first, last):
        for i in range(first, last):
            for j in range(i + 1):
                at = (i, j % cols, j // cols)
                copy(p_ref.at[0, 0], grid_ref.at[at], line_send.at[0, 0], grid_recv.at[at], row, partner).wait_recv()

    def wait_own():
        for k in range(1, cols):
            c = (col + k) % cols
            copy(bulk, own_ref.at[c], own_send.at[k], own_recv.at[c], row, partner).wait_recv()

    results = (low0_ref, inv0_ref, low1_ref, inv1_ref)

    def result_copy(k):
        return copy(results[k], results[k], result_send.at[k], result_recv.at[k], row, partner)

    start = lambda move: move.start()
    done = lambda move: move.wait_send()
    keep = pltpu.make_async_copy(bulk, own_ref.at[col], local_sem.at[0])
    keep_across = pltpu.make_async_copy(bulk, across_ref.at[row // cols, col], local_sem.at[1])
    source = col == row % cols

    line_copies(start)
    keep.start()

    @pl.when(source)
    def _():
        keep_across.start()

    @pl.when(relays)
    def _():
        spread_copies(0, PT, start, True)
        spread_copies(PT, count, start, True)
        column_copies(start)
        own_copies(start)
        cross(start, True)

    @pl.when(works)
    def _():
        wait_grid(0, PT)
        column_copies(start)
        own_copies(start)
        factor_first(cols, tile, grid_ref, low0_ref, inv0_ref, work_ref, up_ref)
        wait_grid(PT, count)
        factor_rest(cols, tile, grid_ref, low0_ref, inv0_ref)
        factor_second(cols, tile, grid_ref, low0_ref, low1_ref, inv1_ref, work_ref, up_ref)
        for k in range(4):
            result_copy(k).start()
        for k in range(4):
            result_copy(k).wait_send()
        for g in range(groups):
            for c in range(cols):
                copy(bulk, across_ref.at[g, c], own_send.at[0], across_recv.at[g, c], row, partner).wait_recv()

    line_copies(done)

    @pl.when(relays)
    def _():
        spread_copies(0, count, done, False)
        cross(done, False)
        for k in range(4):
            result_copy(k).wait_recv()

    column_copies(done)
    own_copies(done)
    wait_own()
    keep.wait()

    @pl.when(source)
    def _():
        keep_across.wait()


def span_of(tile):
    return lambda i, j=None: slice(i * tile, (i + 1 if j is None else j) * tile)


def load_piece(cols, tile, grid_ref, i, j):
    lane = lax.broadcasted_iota(jnp.int32, (tile, tile), 1)
    sub = lax.broadcasted_iota(jnp.int32, (tile, tile), 0)
    piece = grid_ref[i, j % cols, j // cols, 0:tile]
    if i == j:
        kept = jnp.where(lane <= sub, piece, 0.0)
        piece = kept + jnp.where(lane < sub, piece, 0.0).T
    return piece


def factor_chain(tile, low_ref, inv_ref, work_ref, up_ref):
    span = span_of(tile)
    for t in range(PT):
        factor_tile(low_ref[span(t), span(t)], work_ref, up_ref, inv_ref.at[t])
        low_ref[span(t), span(t)] = up_ref[...].T
        if t + 1 < PT:
            solved = dot_nt(low_ref[span(t + 1, PT), span(t)], inv_ref[t])
            low_ref[span(t + 1, PT), span(t)] = solved
            for u in range(t + 1, PT):
                low_ref[span(u, PT), span(u)] -= dot_nt(
                    low_ref[span(u, PT), span(t)], low_ref[span(u), span(t)]
                )


def factor_first(cols, tile, grid_ref, low_ref, inv_ref, work_ref, up_ref):
    span = span_of(tile)
    for i in range(PT):
        for j in range(PT):
            if j > i:
                low_ref[span(i), span(j)] = jnp.zeros((tile, tile), jnp.float32)
            else:
                low_ref[span(i), span(j)] = load_piece(cols, tile, grid_ref, i, j)
    factor_chain(tile, low_ref, inv_ref, work_ref, up_ref)


def factor_rest(cols, tile, grid_ref, low_ref, inv_ref):
    span = span_of(tile)
    rest = slice(PT * tile, 2 * PT * tile)
    for i in range(PT, 2 * PT):
        for j in range(PT):
            low_ref[span(i), span(j)] = load_piece(cols, tile, grid_ref, i, j)
    for t in range(PT):
        value = low_ref[rest, span(t)]
        if t:
            value = value - dot_nt(low_ref[rest, span(0, t)], low_ref[span(t), span(0, t)])
        low_ref[rest, span(t)] = dot_nt(value, inv_ref[t])


def factor_second(cols, tile, grid_ref, before_ref, low_ref, inv_ref, work_ref, up_ref):
    span = span_of(tile)
    for i in range(PT):
        for j in range(PT):
            if j > i:
                low_ref[span(i), span(j)] = jnp.zeros((tile, tile), jnp.float32)
                continue
            piece = load_piece(cols, tile, grid_ref, PT + i, PT + j)
            left = before_ref[span(PT + i), :]
            right = before_ref[span(PT + j), :]
            at = PT + j
            mark = grid_ref[PT + i, at % cols, at // cols, tile : tile + 1]
            piece = piece - jnp.where(mark > 0.5, dot_nt_coarse(left, right), dot_nt(left, right))
            low_ref[span(i), span(j)] = piece
    factor_chain(tile, low_ref, inv_ref, work_ref, up_ref)


def exchange(payload, rows, cols):
    tile_rows, slots, height, tile = payload.shape
    count = 2 * PT
    groups = rows // cols
    skip = count // rows
    dims = (rows, cols, slots, skip, tile)
    part = (tile_rows - skip, slots, height, tile)
    vmem = pl.BlockSpec(memory_space=pltpu.VMEM)
    hbm = pl.BlockSpec(memory_space=pltpu.HBM)
    f32 = lambda *shape: jax.ShapeDtypeStruct(shape, jnp.float32)
    dma = pltpu.SemaphoreType.DMA
    return pl.pallas_call(
        lambda *refs: exchange_kernel(dims, *refs),
        out_shape=(
            f32(cols, *part),
            f32(groups, cols, *part),
            f32(count * tile, PT * tile),
            f32(PT, tile, tile),
            f32(PT * tile, PT * tile),
            f32(PT, tile, tile),
        ),
        in_specs=[vmem],
        out_specs=(hbm, hbm, vmem, vmem, vmem, vmem),
        scratch_shapes=[
            pltpu.VMEM((count, cols, slots, height, tile), jnp.float32),
            pltpu.VMEM((count // 2, 2, slots, height, tile), jnp.float32),
            pltpu.VMEM((tile, 2 * tile), jnp.float32),
            pltpu.VMEM((tile, tile), jnp.float32),
            dma((slots, rows // 2)),
            dma((count // 2, 2, slots)),
            dma((count // 2, 2, slots, 2, cols // 2)),
            dma((count, cols, slots)),
            dma((cols,)),
            dma((cols,)),
            dma((rows // 2,)),
            dma((groups, cols)),
            dma((groups, cols)),
            dma((4,)),
            dma((4,)),
            dma((2,)),
        ],
        compiler_params=pltpu.CompilerParams(has_side_effects=True, vmem_limit_bytes=32 * 1024 * 1024),
        name="exchange",
    )(payload)


def solve_kernel(tile, skip, ids_ref, order_ref, panel_ref, low0_ref, inv0_ref, low1_ref, inv1_ref,
                 high_ref, rest_ref, low_h, low_l, inv_h, inv_l):
    count = 2 * PT
    width = PT * tile
    rows = panel_ref.shape[1]
    col_count = panel_ref.shape[0]
    group = pl.program_id(0)

    def span(i, j=None):
        return slice(i * tile, (i + 1 if j is None else j) * tile)

    @pl.when(group == 0)
    def _():
        for i in range(count):
            low_h[span(i), :width], low_l[span(i), :width] = split(low0_ref[span(i), :])
        for i in range(PT):
            at = PT + i
            low_h[span(at), width:], low_l[span(at), width:] = split(low1_ref[span(i), :])
            low_h[span(i), width:] = jnp.zeros((tile, width), jnp.bfloat16)
            low_l[span(i), width:] = jnp.zeros((tile, width), jnp.bfloat16)
            inv_h[i], inv_l[i] = split(inv0_ref[i])
            inv_h[at], inv_l[at] = split(inv1_ref[i])

    def flat(value):
        return value.reshape(rows * tile, tile)

    mine = slice(skip * tile, (skip + rows) * tile)

    for t in range(count):
        first = t // PT * PT
        slot = t // col_count
        owner = order_ref[t]
        value = flat(panel_ref[owner, :, slot, :tile, :])
        if first:
            left = (high_ref[0, mine, :width], rest_ref[0, mine, :width])
            right = (low_h[span(t), :width], low_l[span(t), :width])
            coarse = dot_bf16(left[0], right[0])
            exact = coarse + (dot_bf16(left[0], right[1]) + dot_bf16(left[1], right[0]))
            mark = panel_ref[owner, :, slot, tile : tile + 1, :]
            mark = flat(jnp.broadcast_to(mark, (rows, tile, tile)))
            value = value - jnp.where(mark > 0.5, coarse, exact)
        if t > first:
            value = value - dot_pairs(
                (high_ref[0, mine, span(first, t)], rest_ref[0, mine, span(first, t)]),
                (low_h[span(t), span(first, t)], low_l[span(t), span(first, t)]),
            )
        high_ref[0, mine, span(t)], rest_ref[0, mine, span(t)] = split(
            dot_pairs(split(value), (inv_h[t], inv_l[t]))
        )

    row = ids_ref[group]

    @pl.when(row < count)
    def _():
        base = pl.multiple_of(jnp.minimum(row, count - 1) * tile, tile)
        high_ref[0, :tile, :] = low_h[pl.ds(base, tile), :]
        rest_ref[0, :tile, :] = low_l[pl.ds(base, tile), :]


def solve_panels(ids, order, panels, factors, groups, skip):
    col_count = panels.shape[0] // groups
    _, rows, slots, height, tile = panels.shape
    count = 2 * PT
    full = count * tile
    keep = lambda n: (lambda g, *refs: (0,) * n)
    out_spec = pl.BlockSpec((1, (skip + rows) * tile, full), lambda g, *refs: (g, 0, 0))
    out_shape = jax.ShapeDtypeStruct((groups, (skip + rows) * tile, full), jnp.bfloat16)
    return pl.pallas_call(
        lambda *refs: solve_kernel(tile, skip, *refs),
        grid_spec=pltpu.PrefetchScalarGridSpec(
            num_scalar_prefetch=2,
            grid=(groups,),
            in_specs=[
                pl.BlockSpec((col_count, rows, slots, height, tile), lambda g, *refs: (g, 0, 0, 0, 0))
            ]
            + [pl.BlockSpec(f.shape, keep(len(f.shape))) for f in factors],
            out_specs=(out_spec, out_spec),
            scratch_shapes=[
                pltpu.VMEM((full, full), jnp.bfloat16),
                pltpu.VMEM((full, full), jnp.bfloat16),
                pltpu.VMEM((count, tile, tile), jnp.bfloat16),
                pltpu.VMEM((count, tile, tile), jnp.bfloat16),
            ],
        ),
        out_shape=(out_shape, out_shape),
        compiler_params=pltpu.CompilerParams(vmem_limit_bytes=56 * 1024 * 1024),
        cost_estimate=pl.CostEstimate(
            flops=groups * 4_000_000_000, bytes_accessed=groups * 6_000_000, transcendentals=0
        ),
        name="solve_panels",
    )(ids, order, panels, *factors)


def update_kernel(tile, groups, rows_ref, cols_ref, marks_ref, raw_ref, left_h, left_l, right_h, right_l, out_ref):
    count = 2 * PT
    b = pl.program_id(0)
    j = cols_ref[b]
    base = pl.multiple_of(jnp.minimum(j, count - 1) * tile, tile)
    at = pl.multiple_of(b // groups * tile, tile)
    group = b % groups

    def rounded(value):
        return value.astype(jnp.bfloat16).astype(jnp.float32)

    def tile_row(a):
        i = rows_ref[a]
        mark = marks_ref[a * pl.num_programs(0) + b]
        mine = slice(a * tile, (a + 1) * tile)

        @pl.when(i < j)
        def _():
            out_ref[a, 0] = jnp.zeros((tile, tile), jnp.float32)

        @pl.when((i >= j) & (j < count))
        def _():
            high = left_h[0, mine, pl.ds(base, tile)].astype(jnp.float32)
            rest = left_l[0, mine, pl.ds(base, tile)].astype(jnp.float32)
            out_ref[a, 0] = high + jnp.where(mark == 1, 0.0, rest)

        @pl.when((i >= j) & (j >= count) & (mark == 1))
        def _():
            other = right_h[group, pl.ds(at, tile), :]
            out_ref[a, 0] = rounded(rounded(raw_ref[a, 0]) - dot_bf16(left_h[0, mine, :], other))

        @pl.when((i >= j) & (j >= count) & (mark != 1))
        def _():
            high = right_h[group, pl.ds(at, tile), :]
            rest = right_l[group, pl.ds(at, tile), :]
            out_ref[a, 0] = raw_ref[a, 0] - dot_pairs(
                (left_h[0, mine, :], left_l[0, mine, :]), (high, rest)
            )

    for a in range(raw_ref.shape[0]):
        tile_row(a)


def update_tiles(row_ids, col_ids, marks, tiles, left, right):
    rows, cols, tile, _ = tiles.shape
    groups = right[0].shape[0]
    whole = lambda b, *refs: (0, 0, 0)
    each = pl.BlockSpec((rows, 1, tile, tile), lambda b, *refs: (0, b, 0, 0))
    return pl.pallas_call(
        lambda *refs: update_kernel(tile, groups, *refs),
        grid_spec=pltpu.PrefetchScalarGridSpec(
            num_scalar_prefetch=3,
            grid=(cols,),
            in_specs=[each] + [pl.BlockSpec(v.shape, whole) for v in (*left, *right)],
            out_specs=each,
        ),
        out_shape=jax.ShapeDtypeStruct(tiles.shape, jnp.float32),
        compiler_params=pltpu.CompilerParams(vmem_limit_bytes=60 * 1024 * 1024),
        name="update_tiles",
    )(row_ids, col_ids, marks.reshape(-1), tiles, *left, *right)


def on_device(matrix, flags):
    row_count = lax.axis_size("row")
    col_count = lax.axis_size("col")
    row_index = lax.axis_index("row")
    col_index = lax.axis_index("col")
    tile_rows = matrix.shape[0]
    tile_cols = matrix.shape[2]
    tile = matrix.shape[4]
    count = 2 * PT
    slots = count // col_count
    groups = row_count // col_count
    tiles = matrix.reshape(tile_rows, tile_cols, tile, tile)
    marks = flags.reshape(tile_rows, tile_cols)
    row_ids = jnp.arange(tile_rows, dtype=jnp.int32) * row_count + row_index
    col_ids = jnp.arange(tile_cols, dtype=jnp.int32) * col_count + col_index

    head = tiles[:, :slots]
    head_marks = (marks[:, :slots] == 1)[:, :, None, None]
    stored = jnp.where(head_marks, lax.reduce_precision(head, 8, 7), head)
    tags = jnp.broadcast_to(head_marks.astype(jnp.float32), (tile_rows, slots, 8, tile))
    payload = jnp.concatenate([stored, tags], axis=2)

    own, across, *factors = exchange(payload, row_count, col_count)
    skip = count // row_count
    columns = jnp.arange(count, dtype=jnp.int32)
    across = across.reshape(groups * col_count, *across.shape[2:])
    left = solve_panels(row_ids[:1], columns % col_count, own, factors, 1, skip)
    right = solve_panels(col_ids[:groups], columns % col_count, across, factors, groups, skip)
    out = update_tiles(row_ids, col_ids, marks, tiles, left, right)
    return out.reshape(matrix.shape)


def solution(mesh):
    return jax.shard_map(
        on_device,
        mesh=mesh,
        in_specs=(P(None, "row", None, "col", None, None), P(None, "row", None, "col")),
        out_specs=P(None, "row", None, "col", None, None),
        check_vma=False,
    )
```

```python
import jax
import jax.numpy as jnp
from jax import lax
from jax.experimental import pallas as pl
from jax.experimental.pallas import tpu as pltpu
from jax.sharding import PartitionSpec as P

PT = 4
MICRO = 32
NT_DIMS = (((1,), (1,)), ((), ()))
TN_DIMS = (((0,), (0,)), ((), ()))


def dot_nt_coarse(a, b):
    return lax.dot_general(
        a.astype(jnp.bfloat16),
        b.astype(jnp.bfloat16),
        NT_DIMS,
        preferred_element_type=jnp.float32,
    )


def split(value):
    high = value.astype(jnp.bfloat16)
    return high, (value - high.astype(jnp.float32)).astype(jnp.bfloat16)


def dot_bf16(a, b):
    return lax.dot_general(a, b, NT_DIMS, preferred_element_type=jnp.float32)


def split3(value):
    high = value.astype(jnp.bfloat16)
    rest = value - high.astype(jnp.float32)
    mid = rest.astype(jnp.bfloat16)
    return high, mid, (rest - mid.astype(jnp.float32)).astype(jnp.bfloat16)


def wide_nt(a, b):
    ah, am, al = split3(a)
    bh, bm, bl = split3(b)
    left = jnp.concatenate([ah, ah, am, am, ah, al], axis=1)
    right = jnp.concatenate([bh, bm, bh, bm, bl, bh], axis=1)
    return dot_bf16(left, right)


def factor_tile(work_ref, low_ref, upper_ref, inv_ref):
    tile = work_ref.shape[0]
    lanes = lax.broadcasted_iota(jnp.int32, (8, tile), 1)
    subs = lax.broadcasted_iota(jnp.int32, (8, tile), 0)
    parts = MICRO // 8

    def spread(value, k):
        return jnp.broadcast_to(value[k : k + 1, :], (8, tile))

    for base in range(0, tile, MICRO):
        raw = {g: work_ref[base + 8 * g : base + 8 * g + 8, :] for g in range(parts)}
        col, slab, diag = {}, {}, {}
        for g in range(parts):
            for q in range(8 * g + 8):
                col[q, g] = jnp.broadcast_to(raw[g][:, base + q : base + q + 1], (8, tile))
            inside = (lanes >= base) & (lanes < base + MICRO)
            one = (lanes == base + 8 * g + subs).astype(jnp.float32)
            slab[g] = jnp.where(inside, one, raw[g])
            diag[g] = jnp.zeros((8, tile), jnp.float32)
        for q in range(0, MICRO, 2):
            h, k = q // 8, q % 8
            d0 = spread(col[q, h], k)
            e = spread(col[q, h], k + 1)
            d1 = spread(col[q + 1, h], k + 1)
            r0 = lax.rsqrt(d0)
            r1 = lax.rsqrt(d0 * d1 - e * e) * (d0 * r0)
            l10 = e * r0
            l0, l1 = {}, {}
            for g in range(h, parts):
                l0[g] = col[q, g] * r0
                l1[g] = (col[q + 1, g] - l0[g] * l10) * r1
                diag[g] = jnp.where(lanes == base + q, l0[g], jnp.where(lanes == base + q + 1, l1[g], diag[g]))
            for m in range(q + 2, MICRO):
                a0 = spread(l0[m // 8], m % 8)
                a1 = spread(l1[m // 8], m % 8)
                for g in range(m // 8, parts):
                    col[m, g] = col[m, g] - (l0[g] * a0 + l1[g] * a1)
            u0 = spread(slab[h], k) * r0
            u1 = (spread(slab[h], k + 1) - u0 * l10) * r1
            for g in range(h, parts):
                new = slab[g] - (l0[g] * u0 + l1[g] * u1)
                if g == h:
                    old = jnp.where(subs == k, u0, slab[g])
                    new = jnp.where(subs > k + 1, new, jnp.where(subs == k + 1, u1, old))
                slab[g] = new
        for g in range(parts):
            at = slice(base + 8 * g, base + 8 * g + 8)
            under = lanes <= base + 8 * g + subs
            low_ref[at, :] = jnp.where(under, diag[g], 0.0)
            upper_ref[at, :] = jnp.where(lanes >= base + MICRO, slab[g], 0.0)
            inv_ref[at, :] = jnp.where(under, slab[g], 0.0)
        if base + MICRO < tile:
            high, mid, rest = split3(jnp.concatenate([slab[g] for g in range(parts)], axis=0))
            left = jnp.concatenate([high, high, mid, mid, high, rest], axis=0)
            right = jnp.concatenate([high, mid, high, mid, rest, high], axis=0)
            after = slice(base + MICRO, tile)
            outer = lax.dot_general(left, right, TN_DIMS, preferred_element_type=jnp.float32)[after]
            lane = lax.broadcasted_iota(jnp.int32, (tile - base - MICRO, tile), 1)
            inside = (lane >= base) & (lane < base + MICRO)
            work_ref[after, :] = jnp.where(inside, 0.0, work_ref[after, :]) - outer
    low_ref[...] += upper_ref[...].T


def exchange_kernel(dims, p_ref, own_ref, across_ref, low0_ref, inv0_ref, low1_ref, inv1_ref,
                    grid_ref, relay_ref, work_ref, up_ref,
                    line_send, line_recv, spread_send, grid_recv, own_send, own_recv,
                    column_send, across_recv, cross_send, result_send, result_recv, local_sem):
    rows, cols, slots, skip, tile = dims
    count = 2 * PT
    groups = rows // cols
    lines = rows // 2
    row = lax.axis_index("row")
    col = lax.axis_index("col")
    along, side = row // 2, row % 2
    wide, core = col // 2, col % 2
    relays = (row + col) % 2 == 0
    works = (row + col) % 2 == 1
    partner = wide * 2 + 1 - core
    bulk = p_ref.at[skip:]

    def copy(src, dst, send, recv, to_row, to_col):
        return pltpu.make_async_remote_copy(
            src_ref=src, dst_ref=dst, send_sem=send, recv_sem=recv,
            device_id=(to_row, to_col), device_id_type=pl.DeviceIdType.MESH,
        )

    def line_copies(act):
        for s in range(slots):
            for k in range(lines):
                here = (k == along) & (core == side)

                @pl.when((s * cols + col <= row) & (row < count) & jnp.logical_not(here))
                def _():
                    act(copy(p_ref.at[0, s], relay_ref.at[along, core, s], line_send.at[s, k],
                             line_recv.at[along, core, s], 2 * k + side, wide * 2 + side))

    def spread_copies(first, last, act, wait):
        for k in range(first // 2, last // 2):
            for c in range(2):
                for s in range(slots):
                    mine = (k == along) & (core == c)
                    from_col = wide * 2 + c
                    from_row = 2 * k + side
                    need = s * cols + from_col <= from_row

                    def targets(src):
                        for n in range(2):
                            for w in range(cols // 2):
                                act(copy(src, grid_ref.at[from_row, from_col, s],
                                         spread_send.at[k, c, s, n, w],
                                         grid_recv.at[from_row, from_col, s],
                                         2 * along + n, 2 * w + 1 - n))

                    @pl.when(need & mine)
                    def _():
                        targets(p_ref.at[0, s])

                    @pl.when(need & jnp.logical_not(mine))
                    def _():
                        if wait:
                            copy(p_ref.at[0, s], relay_ref.at[k, c, s], line_send.at[s, 0],
                                 line_recv.at[k, c, s], row, partner).wait_recv()
                        targets(relay_ref.at[k, c, s])

    def own_copies(act):
        for k in range(1, cols):
            act(copy(bulk, own_ref.at[col], own_send.at[k], own_recv.at[col], row, (col + k) % cols))

    def column_copies(act):
        for k in range(lines):
            @pl.when(jnp.logical_not((k == along) & (col == row % cols)))
            def _():
                act(copy(bulk, across_ref.at[row // cols, col], column_send.at[k],
                         across_recv.at[row // cols, col], 2 * k + side, row % cols))

    def cross(act, wait):
        near = jnp.clip((along - wide + cols // 4) // (cols // 2), 0, groups - 1)
        for k in range(cols):
            from_col = (wide + k // 2) % (cols // 2) * 2 + (core + k) % 2
            for h in range(groups):
                g = (near + h) % groups
                mine = (g * cols + col == row) & (from_col == col)

                def forward(src):
                    return copy(src, across_ref.at[g, from_col], cross_send.at[g, from_col],
                                across_recv.at[g, from_col], 2 * along + 1 - side, col)

                @pl.when(mine)
                def _():
                    act(forward(bulk))

                @pl.when(jnp.logical_not(mine))
                def _():
                    move = forward(across_ref.at[g, from_col])
                    if wait:
                        move.wait_recv()
                    act(move)

    def wait_grid(first, last):
        for i in range(first, last):
            for j in range(i + 1):
                at = (i, j % cols, j // cols)
                copy(p_ref.at[0, 0], grid_ref.at[at], line_send.at[0, 0], grid_recv.at[at], row, partner).wait_recv()

    def wait_own():
        for k in range(1, cols):
            c = (col + k) % cols
            copy(bulk, own_ref.at[c], own_send.at[k], own_recv.at[c], row, partner).wait_recv()

    results = (low0_ref, inv0_ref, low1_ref, inv1_ref)

    def result_copy(k):
        return copy(results[k], results[k], result_send.at[k], result_recv.at[k], row, partner)

    start = lambda move: move.start()
    done = lambda move: move.wait_send()
    keep = pltpu.make_async_copy(bulk, own_ref.at[col], local_sem.at[0])
    keep_across = pltpu.make_async_copy(bulk, across_ref.at[row // cols, col], local_sem.at[1])
    source = col == row % cols

    line_copies(start)
    keep.start()

    @pl.when(source)
    def _():
        keep_across.start()

    @pl.when(relays)
    def _():
        spread_copies(0, PT, start, True)
        spread_copies(PT, count, start, True)
        column_copies(start)
        own_copies(start)
        cross(start, True)

    @pl.when(works)
    def _():
        wait_grid(0, PT)
        column_copies(start)
        own_copies(start)
        factor_first(cols, tile, grid_ref, low0_ref, inv0_ref, work_ref, up_ref)
        wait_grid(PT, count)
        factor_rest(cols, tile, grid_ref, low0_ref, inv0_ref)
        factor_second(cols, tile, grid_ref, low0_ref, low1_ref, inv1_ref, work_ref, up_ref,
                      lambda: [result_copy(k).start() for k in range(2)])
        for k in range(2, 4):
            result_copy(k).start()
        for k in range(4):
            result_copy(k).wait_send()
        for g in range(groups):
            for c in range(cols):
                copy(bulk, across_ref.at[g, c], own_send.at[0], across_recv.at[g, c], row, partner).wait_recv()

    line_copies(done)

    @pl.when(relays)
    def _():
        spread_copies(0, count, done, False)
        cross(done, False)
        for k in range(4):
            result_copy(k).wait_recv()

    column_copies(done)
    own_copies(done)
    wait_own()
    keep.wait()

    @pl.when(source)
    def _():
        keep_across.wait()


def span_of(tile):
    return lambda i, j=None: slice(i * tile, (i + 1 if j is None else j) * tile)


def load_piece(cols, tile, grid_ref, i, j):
    lane = lax.broadcasted_iota(jnp.int32, (tile, tile), 1)
    sub = lax.broadcasted_iota(jnp.int32, (tile, tile), 0)
    piece = grid_ref[i, j % cols, j // cols, 0:tile]
    if i == j:
        kept = jnp.where(lane <= sub, piece, 0.0)
        piece = kept + jnp.where(lane < sub, piece, 0.0).T
    return piece


def factor_chain(tile, low_ref, inv_ref, work_ref, up_ref):
    span = span_of(tile)
    for t in range(PT):
        pair, half = t // 2, t % 2
        at = span(half)
        work_ref[...] = low_ref[span(t), span(t)]
        factor_tile(work_ref, low_ref.at[span(t), span(t)], up_ref, inv_ref.at[pair, at, at])
        if t + 1 < PT:
            solved = wide_nt(low_ref[span(t + 1, PT), span(t)], inv_ref[pair, at, at])
            low_ref[span(t + 1, PT), span(t)] = solved
            for u in range(t + 1, PT):
                low_ref[span(u, PT), span(u)] -= wide_nt(
                    low_ref[span(u, PT), span(t)], low_ref[span(u), span(t)]
                )
        if half:
            under = wide_nt(inv_ref[pair, at, at], low_ref[span(t), span(t - 1)].T)
            inv_ref[pair, at, span(0)] = -wide_nt(under, inv_ref[pair, span(0), span(0)].T)
            inv_ref[pair, span(0), at] = jnp.zeros((tile, tile), jnp.float32)


def factor_first(cols, tile, grid_ref, low_ref, inv_ref, work_ref, up_ref):
    span = span_of(tile)
    for i in range(PT):
        for j in range(PT):
            if j > i:
                low_ref[span(i), span(j)] = jnp.zeros((tile, tile), jnp.float32)
            else:
                low_ref[span(i), span(j)] = load_piece(cols, tile, grid_ref, i, j)
    factor_chain(tile, low_ref, inv_ref, work_ref, up_ref)


def factor_rest(cols, tile, grid_ref, low_ref, inv_ref):
    span = span_of(tile)
    rest = slice(PT * tile, 2 * PT * tile)
    for i in range(PT, 2 * PT):
        for j in range(PT):
            low_ref[span(i), span(j)] = load_piece(cols, tile, grid_ref, i, j)
    for t in range(PT):
        value = low_ref[rest, span(t)]
        if t:
            value = value - wide_nt(low_ref[rest, span(0, t)], low_ref[span(t), span(0, t)])
        at = span(t % 2)
        low_ref[rest, span(t)] = wide_nt(value, inv_ref[t // 2, at, at])


def factor_second(cols, tile, grid_ref, before_ref, low_ref, inv_ref, work_ref, up_ref, ready):
    span = span_of(tile)
    for i in range(PT):
        for j in range(PT):
            if j > i:
                low_ref[span(i), span(j)] = jnp.zeros((tile, tile), jnp.float32)
                continue
            piece = load_piece(cols, tile, grid_ref, PT + i, PT + j)
            left = before_ref[span(PT + i), :]
            right = before_ref[span(PT + j), :]
            at = PT + j
            mark = grid_ref[PT + i, at % cols, at // cols, tile : tile + 1]
            exact = wide_nt(left[:, : 2 * tile], right[:, : 2 * tile]) + wide_nt(left[:, 2 * tile :], right[:, 2 * tile :])
            piece = piece - jnp.where(mark > 0.5, dot_nt_coarse(left, right), exact)
            low_ref[span(i), span(j)] = piece
    ready()
    factor_chain(tile, low_ref, inv_ref, work_ref, up_ref)


def exchange(payload, rows, cols):
    tile_rows, slots, height, tile = payload.shape
    count = 2 * PT
    groups = rows // cols
    skip = count // rows
    dims = (rows, cols, slots, skip, tile)
    part = (tile_rows - skip, slots, height, tile)
    vmem = pl.BlockSpec(memory_space=pltpu.VMEM)
    hbm = pl.BlockSpec(memory_space=pltpu.HBM)
    f32 = lambda *shape: jax.ShapeDtypeStruct(shape, jnp.float32)
    dma = pltpu.SemaphoreType.DMA
    return pl.pallas_call(
        lambda *refs: exchange_kernel(dims, *refs),
        out_shape=(
            f32(cols, *part),
            f32(groups, cols, *part),
            f32(count * tile, PT * tile),
            f32(PT // 2, 2 * tile, 2 * tile),
            f32(PT * tile, PT * tile),
            f32(PT // 2, 2 * tile, 2 * tile),
        ),
        in_specs=[vmem],
        out_specs=(hbm, hbm, vmem, vmem, vmem, vmem),
        scratch_shapes=[
            pltpu.VMEM((count, cols, slots, height, tile), jnp.float32),
            pltpu.VMEM((count // 2, 2, slots, height, tile), jnp.float32),
            pltpu.VMEM((tile, tile), jnp.float32),
            pltpu.VMEM((tile, tile), jnp.float32),
            dma((slots, rows // 2)),
            dma((count // 2, 2, slots)),
            dma((count // 2, 2, slots, 2, cols // 2)),
            dma((count, cols, slots)),
            dma((cols,)),
            dma((cols,)),
            dma((rows // 2,)),
            dma((groups, cols)),
            dma((groups, cols)),
            dma((4,)),
            dma((4,)),
            dma((2,)),
        ],
        compiler_params=pltpu.CompilerParams(has_side_effects=True, vmem_limit_bytes=32 * 1024 * 1024),
        name="exchange",
    )(payload)


def finish_kernel(row_count, marks_ref, tiles_ref, own_ref, across_ref, low0_hbm, inv0_hbm, low1_hbm, inv1_hbm,
                  out_ref, panel_ref, low0_ref, inv0_ref, low1_ref, inv1_ref, inv_ref, under_ref, cross_h, cross_l,
                  high_ref, rest_ref, raw_ref, new_ref, factor_sem, panel_sem, raw_sem, new_sem):
    groups, col_count, rows, slots, height, tile = across_ref.shape
    tile_rows, tile_cols = tiles_ref.shape[:2]
    count = 2 * PT
    width = PT * tile
    size = rows * tile
    skip = tile_rows - rows
    first_col = count // col_count
    row = lax.axis_index("row")
    col = lax.axis_index("col")
    span = span_of(tile)

    factor_copies = [
        pltpu.make_async_copy(src, dst, factor_sem.at[k])
        for k, (src, dst) in enumerate(
            ((inv0_hbm, inv0_ref), (low0_hbm, low0_ref), (inv1_hbm, inv1_ref), (low1_hbm, low1_ref))
        )
    ]
    panel_copies = [pltpu.make_async_copy(own_ref, panel_ref.at[0], panel_sem.at[0])] + [
        pltpu.make_async_copy(across_ref.at[g], panel_ref.at[1 + g], panel_sem.at[1 + g]) for g in range(groups)
    ]
    raw_copy = pltpu.make_async_copy(tiles_ref, raw_ref, raw_sem)
    for move in (factor_copies[0], panel_copies[0], *factor_copies[1:], *panel_copies[1:], raw_copy):
        move.start()

    def stacked(value):
        high, rest = split(value)
        return jnp.concatenate([high, high, rest], axis=1)

    def dot_stacked(value, weights):
        high, rest = split(value)
        return dot_bf16(jnp.concatenate([high, rest, high], axis=1), weights)

    for move in factor_copies:
        move.wait()
    for k in range(PT // 2):
        inv_ref[k] = stacked(inv0_ref[k])
        inv_ref[PT // 2 + k] = stacked(inv1_ref[k])
    for k, ref in enumerate((low0_ref, low1_ref)):
        for n in range(1, PT // 2):
            under_ref[k, n - 1] = stacked(ref[span(2 * n, 2 * n + 2), span(0, 2)])
    cross_h[...], cross_l[...] = split(low0_ref[span(PT, count), :])

    def solve(group, carry):
        pltpu.make_async_copy(own_ref, panel_ref.at[group], panel_sem.at[group]).wait()

        def column(t):
            return panel_ref[group, t % col_count, :, t // col_count, :tile, :].reshape(size, tile)

        def mark(t):
            value = panel_ref[group, t % col_count, :, t // col_count, tile : tile + 1, :]
            return jnp.broadcast_to(value, (rows, tile, tile)).reshape(size, tile)

        def keep(at, value):
            high_ref[group, :, at], rest_ref[group, :, at] = split(value)

        for p in range(2):
            done = None
            for n in range(PT // 2):
                t = p * PT + 2 * n
                value = jnp.concatenate([column(t), column(t + 1)], axis=1)
                if p:
                    high, rest = high_ref[group, :, :width], rest_ref[group, :, :width]
                    at = span(2 * n, 2 * n + 2)
                    coarse = dot_bf16(high, cross_h[at, :])
                    more = dot_bf16(high, cross_l[at, :]) + dot_bf16(rest, cross_h[at, :])
                    marks = jnp.concatenate([mark(t), mark(t + 1)], axis=1)
                    value = value - (coarse + jnp.where(marks > 0.5, 0.0, more))
                if n:
                    value = value - dot_stacked(done, under_ref[p, n - 1])
                done = dot_stacked(value, inv_ref[p * (PT // 2) + n])
                keep(span(t, t + 2), done)
        return carry

    lax.fori_loop(0, 1 + groups, solve, 0)

    def rounded(value):
        return value.astype(jnp.bfloat16).astype(jnp.float32)

    def write(a, c):
        return pltpu.make_async_copy(new_ref.at[a, c], out_ref.at[a, c], new_sem.at[a, c])

    def panel_tile(a, c):
        base = pl.multiple_of((c * col_count + col) * tile, tile)
        is_bf16 = marks_ref[a, c] == 1
        if a >= skip:
            at = slice((a - skip) * tile, (a - skip + 1) * tile)
            rest = rest_ref[0, at, pl.ds(base, tile)].astype(jnp.float32)
            new_ref[a, c] = high_ref[0, at, pl.ds(base, tile)].astype(jnp.float32) + jnp.where(is_bf16, 0.0, rest)
        if a * row_count < count:
            @pl.when(row < count)
            def _():
                place = pl.multiple_of(jnp.minimum(row, count - 1) * tile, tile)
                inner = c * col_count + col

                @pl.when(inner < PT)
                def _():
                    value = low0_ref[pl.ds(place, tile), pl.ds(pl.multiple_of(jnp.minimum(inner, PT - 1) * tile, tile), tile)]
                    new_ref[a, c] = jnp.where(is_bf16, rounded(value), value)

                @pl.when((inner >= PT) & (row >= PT))
                def _():
                    lower = pl.multiple_of(jnp.clip(row - PT, 0, PT - 1) * tile, tile)
                    across = pl.multiple_of(jnp.clip(inner - PT, 0, PT - 1) * tile, tile)
                    value = low1_ref[pl.ds(lower, tile), pl.ds(across, tile)]
                    new_ref[a, c] = jnp.where(is_bf16, rounded(value), value)

                @pl.when(row < inner)
                def _():
                    new_ref[a, c] = jnp.zeros((tile, tile), jnp.float32)

    zero = jnp.zeros((tile, tile), jnp.float32)
    for a in range(tile_rows):
        for c in range(tile_cols):
            if c < first_col:
                panel_tile(a, c)
                write(a, c).start()
            elif a < c // groups or a < skip:
                new_ref[a, c] = zero
                write(a, c).start()
    raw_copy.wait()
    for b in range(skip, tile_rows):
        at = slice((b - skip) * tile, (b - skip + 1) * tile)
        lower = slice((b - skip) * tile, size)
        high = jnp.concatenate([high_ref[1 + g, at, :] for g in range(groups)], axis=0)
        rest = jnp.concatenate([rest_ref[1 + g, at, :] for g in range(groups)], axis=0)
        coarse = dot_bf16(high_ref[0, lower, :], high)
        more = dot_bf16(high_ref[0, lower, :], rest) + dot_bf16(rest_ref[0, lower, :], high)
        for a in range(b, tile_rows):
            for g in range(groups):
                c = b * groups + g
                if c < first_col:
                    continue
                here = (slice((a - b) * tile, (a - b + 1) * tile), span(g))
                is_bf16 = marks_ref[a, c] == 1
                value = raw_ref[a, c]
                exact = value - (coarse[here] + more[here])
                value = jnp.where(is_bf16, rounded(rounded(value) - coarse[here]), exact)
                new_ref[a, c] = jnp.where(a * row_count + row >= c * col_count + col, value, 0.0)
                write(a, c).start()
    for a in range(tile_rows):
        for c in range(tile_cols):
            write(a, c).wait()


def finish(marks, tiles, own, across, factors, row_count):
    low0, inv0, low1, inv1 = factors
    tile_rows, tile_cols, tile, _ = tiles.shape
    groups, col_count, rows, slots, height, _ = across.shape
    count = 2 * PT
    size = rows * tile
    hbm = pl.BlockSpec(memory_space=pltpu.HBM)
    dma = pltpu.SemaphoreType.DMA
    bf16 = lambda *shape: pltpu.VMEM(shape, jnp.bfloat16)
    f32 = lambda *shape: pltpu.VMEM(shape, jnp.float32)
    return pl.pallas_call(
        lambda *refs: finish_kernel(row_count, *refs),
        out_shape=jax.ShapeDtypeStruct(tiles.shape, jnp.float32),
        in_specs=[pl.BlockSpec(memory_space=pltpu.SMEM)] + [hbm] * 7,
        out_specs=hbm,
        scratch_shapes=[
            f32(1 + groups, col_count, rows, slots, height, tile),
            f32(*low0.shape),
            f32(*inv0.shape),
            f32(*low1.shape),
            f32(*inv1.shape),
            bf16(PT, 2 * tile, 6 * tile),
            bf16(2, PT // 2 - 1, 2 * tile, 6 * tile),
            bf16(PT * tile, PT * tile),
            bf16(PT * tile, PT * tile),
            bf16(1 + groups, size, count * tile),
            bf16(1 + groups, size, count * tile),
            f32(*tiles.shape),
            f32(*tiles.shape),
            dma((4,)),
            dma((1 + groups,)),
            dma(()),
            dma((tile_rows, tile_cols)),
        ],
        compiler_params=pltpu.CompilerParams(vmem_limit_bytes=60 * 1024 * 1024),
        name="finish",
    )(marks, tiles, own, across, low0, inv0, low1, inv1)


def on_device(matrix, flags):
    row_count = lax.axis_size("row")
    col_count = lax.axis_size("col")
    tile_rows = matrix.shape[0]
    tile_cols = matrix.shape[2]
    tile = matrix.shape[4]
    slots = 2 * PT // col_count
    tiles = matrix.reshape(tile_rows, tile_cols, tile, tile)
    marks = flags.reshape(tile_rows, tile_cols)

    head = tiles[:, :slots]
    head_marks = (marks[:, :slots] == 1)[:, :, None, None]
    stored = jnp.where(head_marks, lax.reduce_precision(head, 8, 7), head)
    tags = jnp.broadcast_to(head_marks.astype(jnp.float32), (tile_rows, slots, 8, tile))
    payload = jnp.concatenate([stored, tags], axis=2)

    own, across, *factors = exchange(payload, row_count, col_count)
    out = finish(marks, tiles, own, across, factors, row_count)
    return out.reshape(matrix.shape)


def solution(mesh):
    return jax.shard_map(
        on_device,
        mesh=mesh,
        in_specs=(P(None, "row", None, "col", None, None), P(None, "row", None, "col")),
        out_specs=P(None, "row", None, "col", None, None),
        check_vma=False,
    )
```

```python
import jax
import jax.numpy as jnp
from jax import lax
from jax.experimental import pallas as pl
from jax.experimental.pallas import tpu as pltpu
from jax.sharding import PartitionSpec as P

PT = 4
MICRO = 32
NT_DIMS = (((1,), (1,)), ((), ()))
TN_DIMS = (((0,), (0,)), ((), ()))


def dot_nt_coarse(a, b):
    return lax.dot_general(
        a.astype(jnp.bfloat16),
        b.astype(jnp.bfloat16),
        NT_DIMS,
        preferred_element_type=jnp.float32,
    )


def split(value):
    high = value.astype(jnp.bfloat16)
    return high, (value - high.astype(jnp.float32)).astype(jnp.bfloat16)


def dot_bf16(a, b):
    return lax.dot_general(a, b, NT_DIMS, preferred_element_type=jnp.float32)


def split3(value):
    high = value.astype(jnp.bfloat16)
    rest = value - high.astype(jnp.float32)
    mid = rest.astype(jnp.bfloat16)
    return high, mid, (rest - mid.astype(jnp.float32)).astype(jnp.bfloat16)


def wide_nt(a, b):
    ah, am, al = split3(a)
    bh, bm, bl = split3(b)
    left = jnp.concatenate([ah, ah, am, am, ah, al], axis=1)
    right = jnp.concatenate([bh, bm, bh, bm, bl, bh], axis=1)
    return dot_bf16(left, right)


def factor_tile(work_ref, low_ref, upper_ref, inv_ref):
    tile = work_ref.shape[0]
    lanes = lax.broadcasted_iota(jnp.int32, (8, tile), 1)
    subs = lax.broadcasted_iota(jnp.int32, (8, tile), 0)
    parts = MICRO // 8

    def spread(value, k):
        return jnp.broadcast_to(value[k : k + 1, :], (8, tile))

    for base in range(0, tile, MICRO):
        raw = {g: work_ref[base + 8 * g : base + 8 * g + 8, :] for g in range(parts)}
        col, slab, diag = {}, {}, {}
        for g in range(parts):
            for q in range(8 * g + 8):
                col[q, g] = jnp.broadcast_to(raw[g][:, base + q : base + q + 1], (8, tile))
            inside = (lanes >= base) & (lanes < base + MICRO)
            one = (lanes == base + 8 * g + subs).astype(jnp.float32)
            slab[g] = jnp.where(inside, one, raw[g])
            diag[g] = jnp.zeros((8, tile), jnp.float32)
        for q in range(0, MICRO, 2):
            h, k = q // 8, q % 8
            d0 = spread(col[q, h], k)
            e = spread(col[q, h], k + 1)
            d1 = spread(col[q + 1, h], k + 1)
            r0 = lax.rsqrt(d0)
            r1 = lax.rsqrt(d0 * d1 - e * e) * (d0 * r0)
            l10 = e * r0
            l0, l1 = {}, {}
            for g in range(h, parts):
                l0[g] = col[q, g] * r0
                l1[g] = (col[q + 1, g] - l0[g] * l10) * r1
                diag[g] = jnp.where(lanes == base + q, l0[g], jnp.where(lanes == base + q + 1, l1[g], diag[g]))
            for m in range(q + 2, MICRO):
                a0 = spread(l0[m // 8], m % 8)
                a1 = spread(l1[m // 8], m % 8)
                for g in range(m // 8, parts):
                    col[m, g] = col[m, g] - (l0[g] * a0 + l1[g] * a1)
            u0 = spread(slab[h], k) * r0
            u1 = (spread(slab[h], k + 1) - u0 * l10) * r1
            for g in range(h, parts):
                new = slab[g] - (l0[g] * u0 + l1[g] * u1)
                if g == h:
                    old = jnp.where(subs == k, u0, slab[g])
                    new = jnp.where(subs > k + 1, new, jnp.where(subs == k + 1, u1, old))
                slab[g] = new
        for g in range(parts):
            at = slice(base + 8 * g, base + 8 * g + 8)
            under = lanes <= base + 8 * g + subs
            low_ref[at, :] = jnp.where(under, diag[g], 0.0)
            upper_ref[at, :] = jnp.where(lanes >= base + MICRO, slab[g], 0.0)
            inv_ref[at, :] = jnp.where(under, slab[g], 0.0)
        if base + MICRO < tile:
            high, mid, rest = split3(jnp.concatenate([slab[g] for g in range(parts)], axis=0))
            left = jnp.concatenate([high, high, mid, mid, high, rest], axis=0)
            right = jnp.concatenate([high, mid, high, mid, rest, high], axis=0)
            after = slice(base + MICRO, tile)
            outer = lax.dot_general(left, right, TN_DIMS, preferred_element_type=jnp.float32)[after]
            lane = lax.broadcasted_iota(jnp.int32, (tile - base - MICRO, tile), 1)
            inside = (lane >= base) & (lane < base + MICRO)
            work_ref[after, :] = jnp.where(inside, 0.0, work_ref[after, :]) - outer
    low_ref[...] += upper_ref[...].T


def exchange_kernel(dims, p_ref, panel_ref, through_ref, low0_ref, inv0_ref, low1_ref, inv1_ref,
                    grid_ref, relay_ref, work_ref, up_ref,
                    line_send, line_recv, spread_send, grid_recv, own_send, own_recv,
                    chain_send, chain_recv, side_send, extra_send, across_recv, cross_send, result_send, result_recv, local_sem):
    rows, cols, slots, skip, tile = dims
    count = 2 * PT
    groups = rows // cols
    lines = rows // 2
    row = lax.axis_index("row")
    col = lax.axis_index("col")
    along, side = row // 2, row % 2
    wide, core = col // 2, col % 2
    relays = (row + col) % 2 == 0
    works = (row + col) % 2 == 1
    partner = wide * 2 + 1 - core
    bulk = p_ref.at[skip:]
    own_ref = panel_ref.at[0]
    across_ref = panel_ref.at[1:]

    def copy(src, dst, send, recv, to_row, to_col):
        return pltpu.make_async_remote_copy(
            src_ref=src, dst_ref=dst, send_sem=send, recv_sem=recv,
            device_id=(to_row, to_col), device_id_type=pl.DeviceIdType.MESH,
        )

    def line_copies(act):
        for s in range(slots):
            for k in range(lines):
                here = (k == along) & (core == side)

                @pl.when((s * cols + col <= row) & (row < count) & jnp.logical_not(here))
                def _():
                    act(copy(p_ref.at[0, s], relay_ref.at[along, core, s], line_send.at[s, k],
                             line_recv.at[along, core, s], 2 * k + side, wide * 2 + side))

    def spread_copies(first, last, act, wait):
        for k in range(first // 2, last // 2):
            for c in range(2):
                for s in range(slots):
                    mine = (k == along) & (core == c)
                    from_col = wide * 2 + c
                    from_row = 2 * k + side
                    need = s * cols + from_col <= from_row

                    def targets(src):
                        for n in range(2):
                            for w in range(cols // 2):
                                act(copy(src, grid_ref.at[from_row, from_col, s],
                                         spread_send.at[k, c, s, n, w],
                                         grid_recv.at[from_row, from_col, s],
                                         2 * along + n, 2 * w + 1 - n))

                    @pl.when(need & mine)
                    def _():
                        targets(p_ref.at[0, s])

                    @pl.when(need & jnp.logical_not(mine))
                    def _():
                        if wait:
                            copy(p_ref.at[0, s], relay_ref.at[k, c, s], line_send.at[s, 0],
                                 line_recv.at[k, c, s], row, partner).wait_recv()
                        targets(relay_ref.at[k, c, s])

    wides = cols // 2
    group = row // cols
    direct_here = along % wides == wide

    def own_copies(act, first, last):
        for k in range(first, last):
            to_col = (wide + (k + 1) // 2) % wides * 2 + (core + 1 + k) % 2
            act(copy(bulk, own_ref.at[col], own_send.at[k], own_recv.at[col], row, to_col))

    def extra_copy():
        return copy(bulk, across_ref.at[group, col], extra_send.at[0], across_recv.at[group, col], row, partner)

    def chain_step(d, act, wait, onward, plane):
        for up in (0, 1) if d else (0,):
            k = along + d if up else along - d
            g = (2 * k + side) // cols
            direct = k % wides == wide
            for c in range(2):
                from_col = wide * 2 + c

                def send(src, dst):
                    if onward:
                        if not (d and up):
                            @pl.when(along < lines - 1)
                            def _():
                                act(copy(src, dst, chain_send.at[0, k, c], chain_recv.at[k, c], row + 2, col))

                        if not d or up:
                            @pl.when(along > 0)
                            def _():
                                act(copy(src, dst, chain_send.at[1, k, c], chain_recv.at[k, c], row - 2, col))

                def send_plane(src):
                    if plane:
                        @pl.when(direct)
                        def _():
                            act(copy(src, across_ref.at[g, from_col], cross_send.at[g, from_col],
                                     across_recv.at[g, from_col], 2 * along + 1 - side, col))

                        @pl.when(jnp.logical_not(direct))
                        def _():
                            act(copy(src, across_ref.at[g, from_col], side_send.at[k, c],
                                     across_recv.at[g, from_col], row, (2 * k + side) % cols))

                def send_all(src):
                    @pl.when(direct)
                    def _():
                        send(src, across_ref.at[g, from_col])

                    @pl.when(jnp.logical_not(direct))
                    def _():
                        send(src, through_ref.at[k, c])
                    send_plane(src)

                if not d:
                    @pl.when(core == c)
                    def _():
                        send_all(bulk)

                    @pl.when(core != c)
                    def _():
                        if wait and onward:
                            copy(bulk, own_ref.at[from_col], own_send.at[0], own_recv.at[from_col], row, partner).wait_recv()
                        send_all(own_ref.at[from_col])
                else:
                    @pl.when((k >= 0) & (k < lines) & direct)
                    def _():
                        here = across_ref.at[g, from_col]
                        if wait:
                            copy(bulk, here, own_send.at[0], chain_recv.at[k, c], row, partner).wait_recv()
                        send(here, here)
                        send_plane(here)

                    @pl.when((k >= 0) & (k < lines) & jnp.logical_not(direct))
                    def _():
                        here = through_ref.at[k, c]
                        if wait:
                            copy(bulk, here, own_send.at[0], chain_recv.at[k, c], row, partner).wait_recv()
                        send(here, here)
                        send_plane(here)

    def side_step(d, act, wait):
        for up in (0, 1) if d else (0,):
            k = along + d if up else along - d
            g = (2 * k + side) // cols
            for w in range(1, wides):
                for c in range(2):
                    from_col = (wide + w) % wides * 2 + c

                    @pl.when((k >= 0) & (k < lines) & (k % wides == wide))
                    def _():
                        here = across_ref.at[g, from_col]
                        move = copy(here, here, cross_send.at[g, from_col], across_recv.at[g, from_col],
                                    2 * along + 1 - side, col)
                        if wait:
                            move.wait_recv()
                        act(move)

    def wait_grid(first, last):
        for i in range(first, last):
            for j in range(i + 1):
                at = (i, j % cols, j // cols)
                copy(p_ref.at[0, 0], grid_ref.at[at], line_send.at[0, 0], grid_recv.at[at], row, partner).wait_recv()

    def wait_own(first, last):
        for k in range(first, last):
            c = (wide + (k + 1) // 2) % wides * 2 + (core + 1 + k) % 2
            copy(bulk, own_ref.at[c], own_send.at[k], own_recv.at[c], row, partner).wait_recv()

    results = (low0_ref, inv0_ref, low1_ref, inv1_ref)

    def result_copy(k):
        return copy(results[k], results[k], result_send.at[k], result_recv.at[k], row, partner)

    start = lambda move: move.start()
    done = lambda move: move.wait_send()
    keep = pltpu.make_async_copy(bulk, own_ref.at[col], local_sem.at[0])
    keep_across = pltpu.make_async_copy(bulk, across_ref.at[row // cols, col], local_sem.at[1])
    source = col == row % cols

    line_copies(start)
    keep.start()

    @pl.when(source)
    def _():
        keep_across.start()

    @pl.when(relays)
    def _():
        spread_copies(0, PT, start, True)
        chain_step(0, start, True, True, True)
        spread_copies(PT, count, start, True)
        own_copies(start, 0, 1)
        for d in range(1, lines):
            chain_step(d, start, True, True, True)
            side_step(d - 1, start, True)
            if d == 1:
                own_copies(start, 1, cols - 1)
        side_step(lines - 1, start, True)

    @pl.when(works)
    def _():
        own_copies(start, 0, 1)

        @pl.when(direct_here)
        def _():
            extra_copy().start()
        wait_grid(0, PT)
        factor_first(cols, tile, grid_ref, low0_ref, inv0_ref, work_ref, up_ref)
        own_copies(start, 1, cols - 1)
        wait_grid(PT, count)
        factor_rest(cols, tile, grid_ref, low0_ref, inv0_ref)
        factor_second(cols, tile, grid_ref, low0_ref, low1_ref, inv1_ref, work_ref, up_ref,
                      lambda: [result_copy(k).start() for k in range(2)])
        for k in range(2, 4):
            result_copy(k).start()
        for k in range(4):
            result_copy(k).wait_send()
        for g in range(groups):
            for c in range(cols):
                copy(bulk, across_ref.at[g, c], own_send.at[0], across_recv.at[g, c], row, partner).wait_recv()
        wait_own(0, 1)

        @pl.when(direct_here)
        def _():
            extra_copy().wait_send()

    line_copies(done)

    @pl.when(relays)
    def _():
        spread_copies(0, count, done, False)
        for d in range(lines):
            chain_step(d, done, False, True, True)
            side_step(d, done, False)

        @pl.when(direct_here)
        def _():
            copy(bulk, across_ref.at[group, partner], own_send.at[0], across_recv.at[group, partner], row, partner).wait_recv()
        for k in range(4):
            result_copy(k).wait_recv()

    own_copies(done, 0, cols - 1)
    wait_own(1, cols - 1)
    keep.wait()

    @pl.when(source)
    def _():
        keep_across.wait()


def span_of(tile):
    return lambda i, j=None: slice(i * tile, (i + 1 if j is None else j) * tile)


def load_piece(cols, tile, grid_ref, i, j):
    lane = lax.broadcasted_iota(jnp.int32, (tile, tile), 1)
    sub = lax.broadcasted_iota(jnp.int32, (tile, tile), 0)
    piece = grid_ref[i, j % cols, j // cols, 0:tile]
    if i == j:
        kept = jnp.where(lane <= sub, piece, 0.0)
        piece = kept + jnp.where(lane < sub, piece, 0.0).T
    return piece


def factor_chain(tile, low_ref, inv_ref, work_ref, up_ref):
    span = span_of(tile)
    for t in range(PT):
        pair, half = t // 2, t % 2
        at = span(half)
        work_ref[...] = low_ref[span(t), span(t)]
        factor_tile(work_ref, low_ref.at[span(t), span(t)], up_ref, inv_ref.at[pair, at, at])
        if t + 1 < PT:
            solved = wide_nt(low_ref[span(t + 1, PT), span(t)], inv_ref[pair, at, at])
            low_ref[span(t + 1, PT), span(t)] = solved
            for u in range(t + 1, PT):
                low_ref[span(u, PT), span(u)] -= wide_nt(
                    low_ref[span(u, PT), span(t)], low_ref[span(u), span(t)]
                )
        if half:
            under = wide_nt(inv_ref[pair, at, at], low_ref[span(t), span(t - 1)].T)
            inv_ref[pair, at, span(0)] = -wide_nt(under, inv_ref[pair, span(0), span(0)].T)
            inv_ref[pair, span(0), at] = jnp.zeros((tile, tile), jnp.float32)


def factor_first(cols, tile, grid_ref, low_ref, inv_ref, work_ref, up_ref):
    span = span_of(tile)
    for i in range(PT):
        for j in range(PT):
            if j > i:
                low_ref[span(i), span(j)] = jnp.zeros((tile, tile), jnp.float32)
            else:
                low_ref[span(i), span(j)] = load_piece(cols, tile, grid_ref, i, j)
    factor_chain(tile, low_ref, inv_ref, work_ref, up_ref)


def factor_rest(cols, tile, grid_ref, low_ref, inv_ref):
    span = span_of(tile)
    rest = slice(PT * tile, 2 * PT * tile)
    for i in range(PT, 2 * PT):
        for j in range(PT):
            low_ref[span(i), span(j)] = load_piece(cols, tile, grid_ref, i, j)
    for t in range(PT):
        value = low_ref[rest, span(t)]
        if t:
            value = value - wide_nt(low_ref[rest, span(0, t)], low_ref[span(t), span(0, t)])
        at = span(t % 2)
        low_ref[rest, span(t)] = wide_nt(value, inv_ref[t // 2, at, at])


def factor_second(cols, tile, grid_ref, before_ref, low_ref, inv_ref, work_ref, up_ref, ready):
    span = span_of(tile)
    for i in range(PT):
        for j in range(PT):
            if j > i:
                low_ref[span(i), span(j)] = jnp.zeros((tile, tile), jnp.float32)
                continue
            piece = load_piece(cols, tile, grid_ref, PT + i, PT + j)
            left = before_ref[span(PT + i), :]
            right = before_ref[span(PT + j), :]
            at = PT + j
            mark = grid_ref[PT + i, at % cols, at // cols, tile : tile + 1]
            exact = wide_nt(left[:, : 2 * tile], right[:, : 2 * tile]) + wide_nt(left[:, 2 * tile :], right[:, 2 * tile :])
            piece = piece - jnp.where(mark > 0.5, dot_nt_coarse(left, right), exact)
            low_ref[span(i), span(j)] = piece
    ready()
    factor_chain(tile, low_ref, inv_ref, work_ref, up_ref)


def exchange(payload, rows, cols):
    tile_rows, slots, height, tile = payload.shape
    count = 2 * PT
    groups = rows // cols
    skip = count // rows
    dims = (rows, cols, slots, skip, tile)
    part = (tile_rows - skip, slots, height, tile)
    vmem = pl.BlockSpec(memory_space=pltpu.VMEM)
    hbm = pl.BlockSpec(memory_space=pltpu.HBM)
    f32 = lambda *shape: jax.ShapeDtypeStruct(shape, jnp.float32)
    dma = pltpu.SemaphoreType.DMA
    return pl.pallas_call(
        lambda *refs: exchange_kernel(dims, *refs),
        out_shape=(
            f32(1 + groups, cols, *part),
            f32(rows // 2, 2, *part),
            f32(count * tile, PT * tile),
            f32(PT // 2, 2 * tile, 2 * tile),
            f32(PT * tile, PT * tile),
            f32(PT // 2, 2 * tile, 2 * tile),
        ),
        in_specs=[vmem],
        out_specs=(hbm, hbm, vmem, vmem, vmem, vmem),
        scratch_shapes=[
            pltpu.VMEM((count, cols, slots, height, tile), jnp.float32),
            pltpu.VMEM((count // 2, 2, slots, height, tile), jnp.float32),
            pltpu.VMEM((tile, tile), jnp.float32),
            pltpu.VMEM((tile, tile), jnp.float32),
            dma((slots, rows // 2)),
            dma((count // 2, 2, slots)),
            dma((count // 2, 2, slots, 2, cols // 2)),
            dma((count, cols, slots)),
            dma((cols,)),
            dma((cols,)),
            dma((2, rows // 2, 2)),
            dma((rows // 2, 2)),
            dma((rows // 2, 2)),
            dma((1,)),
            dma((groups, cols)),
            dma((groups, cols)),
            dma((4,)),
            dma((4,)),
            dma((2,)),
        ],
        compiler_params=pltpu.CompilerParams(has_side_effects=True, vmem_limit_bytes=32 * 1024 * 1024),
        name="exchange",
    )(payload)


def finish_kernel(row_count, marks_ref, tiles_ref, panel_ref, low0_ref, inv0_ref, low1_ref, inv1_ref,
                  out_ref, inv_ref, under_ref, cross_h, cross_l, high_ref, rest_ref, new_ref, new_sem):
    groups, col_count, rows, slots, height, tile = panel_ref.shape
    groups -= 1
    tile_rows, tile_cols = tiles_ref.shape[:2]
    count = 2 * PT
    width = PT * tile
    size = rows * tile
    skip = tile_rows - rows
    first_col = count // col_count
    row = lax.axis_index("row")
    col = lax.axis_index("col")
    span = span_of(tile)

    def stacked(value):
        high, rest = split(value)
        return jnp.concatenate([high, high, rest], axis=1)

    def dot_stacked(value, weights):
        high, rest = split(value)
        return dot_bf16(jnp.concatenate([high, rest, high], axis=1), weights)

    for k in range(PT // 2):
        inv_ref[k] = stacked(inv0_ref[k])
        inv_ref[PT // 2 + k] = stacked(inv1_ref[k])
    for k, ref in enumerate((low0_ref, low1_ref)):
        for n in range(1, PT // 2):
            under_ref[k, n - 1] = stacked(ref[span(2 * n, 2 * n + 2), span(0, 2)])
    cross_h[...], cross_l[...] = split(low0_ref[span(PT, count), :])

    def solve(group, carry):
        def column(t):
            return panel_ref[group, t % col_count, :, t // col_count, :tile, :].reshape(size, tile)

        def mark(t):
            value = panel_ref[group, t % col_count, :, t // col_count, tile : tile + 1, :]
            return jnp.broadcast_to(value, (rows, tile, tile)).reshape(size, tile)

        def keep(at, value):
            high_ref[group, :, at], rest_ref[group, :, at] = split(value)

        for p in range(2):
            done = None
            for n in range(PT // 2):
                t = p * PT + 2 * n
                value = jnp.concatenate([column(t), column(t + 1)], axis=1)
                if p:
                    high, rest = high_ref[group, :, :width], rest_ref[group, :, :width]
                    at = span(2 * n, 2 * n + 2)
                    coarse = dot_bf16(high, cross_h[at, :])
                    more = dot_bf16(high, cross_l[at, :]) + dot_bf16(rest, cross_h[at, :])
                    marks = jnp.concatenate([mark(t), mark(t + 1)], axis=1)
                    value = value - (coarse + jnp.where(marks > 0.5, 0.0, more))
                if n:
                    value = value - dot_stacked(done, under_ref[p, n - 1])
                done = dot_stacked(value, inv_ref[p * (PT // 2) + n])
                keep(span(t, t + 2), done)
        return carry

    lax.fori_loop(0, 1 + groups, solve, 0)

    def rounded(value):
        return value.astype(jnp.bfloat16).astype(jnp.float32)

    def write(a, c):
        return pltpu.make_async_copy(new_ref.at[a, c], out_ref.at[a, c], new_sem.at[a, c])

    def panel_tile(a, c):
        base = pl.multiple_of((c * col_count + col) * tile, tile)
        is_bf16 = marks_ref[a, c] == 1
        if a >= skip:
            at = slice((a - skip) * tile, (a - skip + 1) * tile)
            rest = rest_ref[0, at, pl.ds(base, tile)].astype(jnp.float32)
            new_ref[a, c] = high_ref[0, at, pl.ds(base, tile)].astype(jnp.float32) + jnp.where(is_bf16, 0.0, rest)
        if a * row_count < count:
            @pl.when(row < count)
            def _():
                place = pl.multiple_of(jnp.minimum(row, count - 1) * tile, tile)
                inner = c * col_count + col

                @pl.when(inner < PT)
                def _():
                    value = low0_ref[pl.ds(place, tile), pl.ds(pl.multiple_of(jnp.minimum(inner, PT - 1) * tile, tile), tile)]
                    new_ref[a, c] = jnp.where(is_bf16, rounded(value), value)

                @pl.when((inner >= PT) & (row >= PT))
                def _():
                    lower = pl.multiple_of(jnp.clip(row - PT, 0, PT - 1) * tile, tile)
                    across = pl.multiple_of(jnp.clip(inner - PT, 0, PT - 1) * tile, tile)
                    value = low1_ref[pl.ds(lower, tile), pl.ds(across, tile)]
                    new_ref[a, c] = jnp.where(is_bf16, rounded(value), value)

                @pl.when(row < inner)
                def _():
                    new_ref[a, c] = jnp.zeros((tile, tile), jnp.float32)

    zero = jnp.zeros((tile, tile), jnp.float32)
    for a in range(tile_rows):
        for c in range(tile_cols):
            if c < first_col:
                panel_tile(a, c)
                write(a, c).start()
            elif a < c // groups or a < skip:
                new_ref[a, c] = zero
                write(a, c).start()
    for b in range(skip, tile_rows):
        at = slice((b - skip) * tile, (b - skip + 1) * tile)
        lower = slice((b - skip) * tile, size)
        high = jnp.concatenate([high_ref[1 + g, at, :] for g in range(groups)], axis=0)
        rest = jnp.concatenate([rest_ref[1 + g, at, :] for g in range(groups)], axis=0)
        coarse = dot_bf16(high_ref[0, lower, :], high)
        more = dot_bf16(high_ref[0, lower, :], rest) + dot_bf16(rest_ref[0, lower, :], high)
        for a in range(b, tile_rows):
            for g in range(groups):
                c = b * groups + g
                if c < first_col:
                    continue
                here = (slice((a - b) * tile, (a - b + 1) * tile), span(g))
                is_bf16 = marks_ref[a, c] == 1
                value = tiles_ref[a, c]
                exact = value - (coarse[here] + more[here])
                value = jnp.where(is_bf16, rounded(rounded(value) - coarse[here]), exact)
                new_ref[a, c] = jnp.where(a * row_count + row >= c * col_count + col, value, 0.0)
                write(a, c).start()
    for a in range(tile_rows):
        for c in range(tile_cols):
            write(a, c).wait()


def finish(marks, tiles, panels, factors, row_count):
    low0, inv0, low1, inv1 = factors
    tile_rows, tile_cols, tile, _ = tiles.shape
    groups, col_count, rows, slots, height, _ = panels.shape
    groups -= 1
    count = 2 * PT
    size = rows * tile
    hbm = pl.BlockSpec(memory_space=pltpu.HBM)
    vmem = pl.BlockSpec(memory_space=pltpu.VMEM)
    dma = pltpu.SemaphoreType.DMA
    bf16 = lambda *shape: pltpu.VMEM(shape, jnp.bfloat16)
    f32 = lambda *shape: pltpu.VMEM(shape, jnp.float32)
    held = 2 * tiles.size + panels.size + low0.size + inv0.size + low1.size + inv1.size
    held += (1 + groups) * size * count * tile + 2 * PT * tile * PT * tile
    return pl.pallas_call(
        lambda *refs: finish_kernel(row_count, *refs),
        out_shape=jax.ShapeDtypeStruct(tiles.shape, jnp.float32),
        in_specs=[pl.BlockSpec(memory_space=pltpu.SMEM)] + [vmem] * 6,
        out_specs=hbm,
        scratch_shapes=[
            bf16(PT, 2 * tile, 6 * tile),
            bf16(2, PT // 2 - 1, 2 * tile, 6 * tile),
            bf16(PT * tile, PT * tile),
            bf16(PT * tile, PT * tile),
            bf16(1 + groups, size, count * tile),
            bf16(1 + groups, size, count * tile),
            f32(*tiles.shape),
            dma((tile_rows, tile_cols)),
        ],
        compiler_params=pltpu.CompilerParams(vmem_limit_bytes=4 * held + 12 * 1024 * 1024),
        name="finish",
    )(marks, tiles, panels, low0, inv0, low1, inv1)


def on_device(matrix, flags):
    row_count = lax.axis_size("row")
    col_count = lax.axis_size("col")
    tile_rows = matrix.shape[0]
    tile_cols = matrix.shape[2]
    tile = matrix.shape[4]
    slots = 2 * PT // col_count
    tiles = matrix.reshape(tile_rows, tile_cols, tile, tile)
    marks = flags.reshape(tile_rows, tile_cols)

    head = tiles[:, :slots]
    head_marks = (marks[:, :slots] == 1)[:, :, None, None]
    stored = jnp.where(head_marks, lax.reduce_precision(head, 8, 7), head)
    tags = jnp.broadcast_to(head_marks.astype(jnp.float32), (tile_rows, slots, 8, tile))
    payload = jnp.concatenate([stored, tags], axis=2)

    panels, _, *factors = exchange(payload, row_count, col_count)
    out = finish(marks, tiles, panels, factors, row_count)
    return out.reshape(matrix.shape)


def solution(mesh):
    return jax.shard_map(
        on_device,
        mesh=mesh,
        in_specs=(P(None, "row", None, "col", None, None), P(None, "row", None, "col")),
        out_specs=P(None, "row", None, "col", None, None),
        check_vma=False,
    )
```

```python
import jax
import jax.numpy as jnp
from jax import lax
from jax.experimental import pallas as pl
from jax.experimental.pallas import tpu as pltpu
from jax.sharding import PartitionSpec as P

PT = 4
MICRO = 32
NT_DIMS = (((1,), (1,)), ((), ()))
TN_DIMS = (((0,), (0,)), ((), ()))


def dot_nt_coarse(a, b):
    return lax.dot_general(
        a.astype(jnp.bfloat16),
        b.astype(jnp.bfloat16),
        NT_DIMS,
        preferred_element_type=jnp.float32,
    )


def split(value):
    high = value.astype(jnp.bfloat16)
    return high, (value - high.astype(jnp.float32)).astype(jnp.bfloat16)


def dot_bf16(a, b):
    return lax.dot_general(a, b, NT_DIMS, preferred_element_type=jnp.float32)


def split3(value):
    high = value.astype(jnp.bfloat16)
    rest = value - high.astype(jnp.float32)
    mid = rest.astype(jnp.bfloat16)
    return high, mid, (rest - mid.astype(jnp.float32)).astype(jnp.bfloat16)


def wide_nt(a, b):
    ah, am, al = split3(a)
    bh, bm, bl = split3(b)
    left = jnp.concatenate([ah, ah, am, am, ah, al], axis=1)
    right = jnp.concatenate([bh, bm, bh, bm, bl, bh], axis=1)
    return dot_bf16(left, right)


def factor_tile(work_ref, low_ref, upper_ref, inv_ref):
    tile = work_ref.shape[0]
    lanes = lax.broadcasted_iota(jnp.int32, (8, tile), 1)
    subs = lax.broadcasted_iota(jnp.int32, (8, tile), 0)
    parts = MICRO // 8

    def spread(value, k):
        return jnp.broadcast_to(value[k : k + 1, :], (8, tile))

    for base in range(0, tile, MICRO):
        raw = {g: work_ref[base + 8 * g : base + 8 * g + 8, :] for g in range(parts)}
        col, slab, diag = {}, {}, {}
        for g in range(parts):
            for q in range(8 * g + 8):
                col[q, g] = jnp.broadcast_to(raw[g][:, base + q : base + q + 1], (8, tile))
            inside = (lanes >= base) & (lanes < base + MICRO)
            one = (lanes == base + 8 * g + subs).astype(jnp.float32)
            slab[g] = jnp.where(inside, one, raw[g])
            diag[g] = jnp.zeros((8, tile), jnp.float32)
        for q in range(0, MICRO, 2):
            h, k = q // 8, q % 8
            d0 = spread(col[q, h], k)
            e = spread(col[q, h], k + 1)
            d1 = spread(col[q + 1, h], k + 1)
            r0 = lax.rsqrt(d0)
            r1 = lax.rsqrt(d0 * d1 - e * e) * (d0 * r0)
            l10 = e * r0
            l0, l1 = {}, {}
            for g in range(h, parts):
                l0[g] = col[q, g] * r0
                l1[g] = (col[q + 1, g] - l0[g] * l10) * r1
                diag[g] = jnp.where(lanes == base + q, l0[g], jnp.where(lanes == base + q + 1, l1[g], diag[g]))
            for m in range(q + 2, MICRO):
                a0 = spread(l0[m // 8], m % 8)
                a1 = spread(l1[m // 8], m % 8)
                for g in range(m // 8, parts):
                    col[m, g] = col[m, g] - (l0[g] * a0 + l1[g] * a1)
            u0 = spread(slab[h], k) * r0
            u1 = (spread(slab[h], k + 1) - u0 * l10) * r1
            for g in range(h, parts):
                new = slab[g] - (l0[g] * u0 + l1[g] * u1)
                if g == h:
                    old = jnp.where(subs == k, u0, slab[g])
                    new = jnp.where(subs > k + 1, new, jnp.where(subs == k + 1, u1, old))
                slab[g] = new
        for g in range(parts):
            at = slice(base + 8 * g, base + 8 * g + 8)
            under = lanes <= base + 8 * g + subs
            low_ref[at, :] = jnp.where(under, diag[g], 0.0)
            upper_ref[at, :] = jnp.where(lanes >= base + MICRO, slab[g], 0.0)
            inv_ref[at, :] = jnp.where(under, slab[g], 0.0)
        if base + MICRO < tile:
            high, mid, rest = split3(jnp.concatenate([slab[g] for g in range(parts)], axis=0))
            left = jnp.concatenate([high, high, mid, mid, high, rest], axis=0)
            right = jnp.concatenate([high, mid, high, mid, rest, high], axis=0)
            after = slice(base + MICRO, tile)
            outer = lax.dot_general(left, right, TN_DIMS, preferred_element_type=jnp.float32)[after]
            lane = lax.broadcasted_iota(jnp.int32, (tile - base - MICRO, tile), 1)
            inside = (lane >= base) & (lane < base + MICRO)
            work_ref[after, :] = jnp.where(inside, 0.0, work_ref[after, :]) - outer
    low_ref[...] += upper_ref[...].T


def exchange_kernel(dims, p_ref, panel_ref, through_ref, low0_ref, inv0_ref, low1_ref, inv1_ref,
                    grid_ref, relay_ref, work_ref, up_ref,
                    line_send, line_recv, spread_send, grid_recv, own_send, own_recv,
                    chain_send, chain_recv, side_send, extra_send, across_recv, cross_send, result_send, result_recv, local_sem):
    rows, cols, slots, skip, tile = dims
    count = 2 * PT
    groups = rows // cols
    lines = rows // 2
    row = lax.axis_index("row")
    col = lax.axis_index("col")
    along, side = row // 2, row % 2
    wide, core = col // 2, col % 2
    relays = (row + col) % 2 == 0
    works = (row + col) % 2 == 1
    partner = wide * 2 + 1 - core
    bulk = p_ref.at[skip:]
    own_ref = panel_ref.at[0]
    across_ref = panel_ref.at[1:]

    def copy(src, dst, send, recv, to_row, to_col):
        return pltpu.make_async_remote_copy(
            src_ref=src, dst_ref=dst, send_sem=send, recv_sem=recv,
            device_id=(to_row, to_col), device_id_type=pl.DeviceIdType.MESH,
        )

    def line_copies(act):
        for s in range(slots):
            for k in range(lines):
                here = (k == along) & (core == side)

                @pl.when((s * cols + col <= row) & (row < count) & jnp.logical_not(here))
                def _():
                    act(copy(p_ref.at[0, s], relay_ref.at[along, core, s], line_send.at[s, k],
                             line_recv.at[along, core, s], 2 * k + side, wide * 2 + side))

    def spread_copies(first, last, act, wait):
        for k in range(first // 2, last // 2):
            for c in range(2):
                for s in range(slots):
                    mine = (k == along) & (core == c)
                    from_col = wide * 2 + c
                    from_row = 2 * k + side
                    need = s * cols + from_col <= from_row

                    def targets(src):
                        for n in range(2):
                            for w in range(cols // 2):
                                act(copy(src, grid_ref.at[from_row, from_col, s],
                                         spread_send.at[k, c, s, n, w],
                                         grid_recv.at[from_row, from_col, s],
                                         2 * along + n, 2 * w + 1 - n))

                    @pl.when(need & mine)
                    def _():
                        targets(p_ref.at[0, s])

                    @pl.when(need & jnp.logical_not(mine))
                    def _():
                        if wait:
                            copy(p_ref.at[0, s], relay_ref.at[k, c, s], line_send.at[s, 0],
                                 line_recv.at[k, c, s], row, partner).wait_recv()
                        targets(relay_ref.at[k, c, s])

    wides = cols // 2
    group = row // cols
    direct_here = along % wides == wide

    def own_copies(act, first, last):
        for k in range(first, last):
            to_col = (wide + (k + 1) // 2) % wides * 2 + (core + 1 + k) % 2
            act(copy(bulk, own_ref.at[col], own_send.at[k], own_recv.at[col], row, to_col))

    middle = bulk.shape[0] // 2
    halves = (slice(0, middle), slice(middle, bulk.shape[0]))

    def extra_copy(h):
        return copy(bulk.at[halves[h]], across_ref.at[group, col, halves[h]], extra_send.at[h],
                    across_recv.at[group, col, h], row, partner)

    def chain_step(d, act, wait, onward, plane):
        for up, h in ((u, h) for u in ((0, 1) if d else (0,)) for h in range(2)):
            part = halves[h]
            k = along + d if up else along - d
            g = (2 * k + side) // cols
            direct = k % wides == wide
            for c in range(2):
                from_col = wide * 2 + c

                def send(src, dst):
                    if onward:
                        if not (d and up):
                            @pl.when(along < lines - 1)
                            def _():
                                act(copy(src, dst, chain_send.at[0, k, c, h], chain_recv.at[k, c, h], row + 2, col))

                        if not d or up:
                            @pl.when(along > 0)
                            def _():
                                act(copy(src, dst, chain_send.at[1, k, c, h], chain_recv.at[k, c, h], row - 2, col))

                def send_plane(src):
                    if plane:
                        @pl.when(direct)
                        def _():
                            act(copy(src, across_ref.at[g, from_col, part], cross_send.at[g, from_col, h],
                                     across_recv.at[g, from_col, h], 2 * along + 1 - side, col))

                        @pl.when(jnp.logical_not(direct))
                        def _():
                            act(copy(src, across_ref.at[g, from_col, part], side_send.at[k, c, h],
                                     across_recv.at[g, from_col, h], row, (2 * k + side) % cols))

                def send_all(src):
                    @pl.when(direct)
                    def _():
                        send(src, across_ref.at[g, from_col, part])

                    @pl.when(jnp.logical_not(direct))
                    def _():
                        send(src, through_ref.at[k, c, part])
                    send_plane(src)

                if not d:
                    @pl.when(core == c)
                    def _():
                        send_all(bulk.at[part])

                    @pl.when(core != c)
                    def _():
                        if wait and onward and h == 0:
                            copy(bulk, own_ref.at[from_col], own_send.at[0], own_recv.at[from_col], row, partner).wait_recv()
                        send_all(own_ref.at[from_col, part])
                else:
                    @pl.when((k >= 0) & (k < lines) & direct)
                    def _():
                        here = across_ref.at[g, from_col, part]
                        if wait:
                            copy(bulk.at[part], here, own_send.at[0], chain_recv.at[k, c, h], row, partner).wait_recv()
                        send(here, here)
                        send_plane(here)

                    @pl.when((k >= 0) & (k < lines) & jnp.logical_not(direct))
                    def _():
                        here = through_ref.at[k, c, part]
                        if wait:
                            copy(bulk.at[part], here, own_send.at[0], chain_recv.at[k, c, h], row, partner).wait_recv()
                        send(here, here)
                        send_plane(here)

    def side_step(d, act, wait):
        for up, h in ((u, h) for u in ((0, 1) if d else (0,)) for h in range(2)):
            part = halves[h]
            k = along + d if up else along - d
            g = (2 * k + side) // cols
            for w in range(1, wides):
                for c in range(2):
                    from_col = (wide + w) % wides * 2 + c

                    @pl.when((k >= 0) & (k < lines) & (k % wides == wide))
                    def _():
                        here = across_ref.at[g, from_col, part]
                        move = copy(here, here, cross_send.at[g, from_col, h], across_recv.at[g, from_col, h],
                                    2 * along + 1 - side, col)
                        if wait:
                            move.wait_recv()
                        act(move)

    def wait_grid(first, last):
        for i in range(first, last):
            for j in range(i + 1):
                at = (i, j % cols, j // cols)
                copy(p_ref.at[0, 0], grid_ref.at[at], line_send.at[0, 0], grid_recv.at[at], row, partner).wait_recv()

    def wait_own(first, last):
        for k in range(first, last):
            c = (wide + (k + 1) // 2) % wides * 2 + (core + 1 + k) % 2
            copy(bulk, own_ref.at[c], own_send.at[k], own_recv.at[c], row, partner).wait_recv()

    results = (low0_ref, inv0_ref, low1_ref, inv1_ref)

    def result_copy(k):
        return copy(results[k], results[k], result_send.at[k], result_recv.at[k], row, partner)

    start = lambda move: move.start()
    done = lambda move: move.wait_send()
    keep = pltpu.make_async_copy(bulk, own_ref.at[col], local_sem.at[0])
    keep_across = pltpu.make_async_copy(bulk, across_ref.at[row // cols, col], local_sem.at[1])
    source = col == row % cols

    line_copies(start)
    keep.start()

    @pl.when(source)
    def _():
        keep_across.start()

    @pl.when(relays)
    def _():
        spread_copies(0, PT, start, True)
        chain_step(0, start, True, True, True)
        spread_copies(PT, count, start, True)
        own_copies(start, 0, 1)
        for d in range(1, lines):
            chain_step(d, start, True, True, True)
            side_step(d - 1, start, True)
            if d == 1:
                own_copies(start, 1, cols - 1)
        side_step(lines - 1, start, True)

    @pl.when(works)
    def _():
        own_copies(start, 0, 1)

        @pl.when(direct_here)
        def _():
            extra_copy(0).start()
            extra_copy(1).start()
        wait_grid(0, PT)
        factor_first(cols, tile, grid_ref, low0_ref, inv0_ref, work_ref, up_ref)
        own_copies(start, 1, cols - 1)
        wait_grid(PT, count)
        factor_rest(cols, tile, grid_ref, low0_ref, inv0_ref)
        factor_second(cols, tile, grid_ref, low0_ref, low1_ref, inv1_ref, work_ref, up_ref,
                      lambda: [result_copy(k).start() for k in range(2)])
        for k in range(2, 4):
            result_copy(k).start()
        for k in range(4):
            result_copy(k).wait_send()
        for g in range(groups):
            for c in range(cols):
                for h in range(2):
                    copy(bulk.at[halves[h]], across_ref.at[g, c, halves[h]], own_send.at[0], across_recv.at[g, c, h],
                         row, partner).wait_recv()
        wait_own(0, 1)

        @pl.when(direct_here)
        def _():
            extra_copy(0).wait_send()
            extra_copy(1).wait_send()

    line_copies(done)

    @pl.when(relays)
    def _():
        spread_copies(0, count, done, False)
        for d in range(lines):
            chain_step(d, done, False, True, True)
            side_step(d, done, False)

        @pl.when(direct_here)
        def _():
            for h in range(2):
                copy(bulk.at[halves[h]], across_ref.at[group, partner, halves[h]], own_send.at[0],
                     across_recv.at[group, partner, h], row, partner).wait_recv()
        for k in range(4):
            result_copy(k).wait_recv()

    own_copies(done, 0, cols - 1)
    wait_own(1, cols - 1)
    keep.wait()

    @pl.when(source)
    def _():
        keep_across.wait()


def span_of(tile):
    return lambda i, j=None: slice(i * tile, (i + 1 if j is None else j) * tile)


def load_piece(cols, tile, grid_ref, i, j):
    lane = lax.broadcasted_iota(jnp.int32, (tile, tile), 1)
    sub = lax.broadcasted_iota(jnp.int32, (tile, tile), 0)
    piece = grid_ref[i, j % cols, j // cols, 0:tile]
    if i == j:
        kept = jnp.where(lane <= sub, piece, 0.0)
        piece = kept + jnp.where(lane < sub, piece, 0.0).T
    return piece


def factor_chain(tile, low_ref, inv_ref, work_ref, up_ref):
    span = span_of(tile)
    for t in range(PT):
        pair, half = t // 2, t % 2
        at = span(half)
        work_ref[...] = low_ref[span(t), span(t)]
        factor_tile(work_ref, low_ref.at[span(t), span(t)], up_ref, inv_ref.at[pair, at, at])
        if t + 1 < PT:
            solved = wide_nt(low_ref[span(t + 1, PT), span(t)], inv_ref[pair, at, at])
            low_ref[span(t + 1, PT), span(t)] = solved
            for u in range(t + 1, PT):
                low_ref[span(u, PT), span(u)] -= wide_nt(
                    low_ref[span(u, PT), span(t)], low_ref[span(u), span(t)]
                )
        if half:
            under = wide_nt(inv_ref[pair, at, at], low_ref[span(t), span(t - 1)].T)
            inv_ref[pair, at, span(0)] = -wide_nt(under, inv_ref[pair, span(0), span(0)].T)
            inv_ref[pair, span(0), at] = jnp.zeros((tile, tile), jnp.float32)


def factor_first(cols, tile, grid_ref, low_ref, inv_ref, work_ref, up_ref):
    span = span_of(tile)
    for i in range(PT):
        for j in range(PT):
            if j > i:
                low_ref[span(i), span(j)] = jnp.zeros((tile, tile), jnp.float32)
            else:
                low_ref[span(i), span(j)] = load_piece(cols, tile, grid_ref, i, j)
    factor_chain(tile, low_ref, inv_ref, work_ref, up_ref)


def factor_rest(cols, tile, grid_ref, low_ref, inv_ref):
    span = span_of(tile)
    rest = slice(PT * tile, 2 * PT * tile)
    for i in range(PT, 2 * PT):
        for j in range(PT):
            low_ref[span(i), span(j)] = load_piece(cols, tile, grid_ref, i, j)
    for t in range(PT):
        value = low_ref[rest, span(t)]
        if t:
            value = value - wide_nt(low_ref[rest, span(0, t)], low_ref[span(t), span(0, t)])
        at = span(t % 2)
        low_ref[rest, span(t)] = wide_nt(value, inv_ref[t // 2, at, at])


def factor_second(cols, tile, grid_ref, before_ref, low_ref, inv_ref, work_ref, up_ref, ready):
    span = span_of(tile)
    for i in range(PT):
        for j in range(PT):
            if j > i:
                low_ref[span(i), span(j)] = jnp.zeros((tile, tile), jnp.float32)
                continue
            piece = load_piece(cols, tile, grid_ref, PT + i, PT + j)
            left = before_ref[span(PT + i), :]
            right = before_ref[span(PT + j), :]
            at = PT + j
            mark = grid_ref[PT + i, at % cols, at // cols, tile : tile + 1]
            exact = wide_nt(left[:, : 2 * tile], right[:, : 2 * tile]) + wide_nt(left[:, 2 * tile :], right[:, 2 * tile :])
            piece = piece - jnp.where(mark > 0.5, dot_nt_coarse(left, right), exact)
            low_ref[span(i), span(j)] = piece
    ready()
    factor_chain(tile, low_ref, inv_ref, work_ref, up_ref)


def exchange(payload, rows, cols):
    tile_rows, slots, height, tile = payload.shape
    count = 2 * PT
    groups = rows // cols
    skip = count // rows
    dims = (rows, cols, slots, skip, tile)
    part = (tile_rows - skip, slots, height, tile)
    vmem = pl.BlockSpec(memory_space=pltpu.VMEM)
    hbm = pl.BlockSpec(memory_space=pltpu.HBM)
    f32 = lambda *shape: jax.ShapeDtypeStruct(shape, jnp.float32)
    dma = pltpu.SemaphoreType.DMA
    return pl.pallas_call(
        lambda *refs: exchange_kernel(dims, *refs),
        out_shape=(
            f32(1 + groups, cols, *part),
            f32(rows // 2, 2, *part),
            f32(count * tile, PT * tile),
            f32(PT // 2, 2 * tile, 2 * tile),
            f32(PT * tile, PT * tile),
            f32(PT // 2, 2 * tile, 2 * tile),
        ),
        in_specs=[vmem],
        out_specs=(hbm, hbm, vmem, vmem, vmem, vmem),
        scratch_shapes=[
            pltpu.VMEM((count, cols, slots, height, tile), jnp.float32),
            pltpu.VMEM((count // 2, 2, slots, height, tile), jnp.float32),
            pltpu.VMEM((tile, tile), jnp.float32),
            pltpu.VMEM((tile, tile), jnp.float32),
            dma((slots, rows // 2)),
            dma((count // 2, 2, slots)),
            dma((count // 2, 2, slots, 2, cols // 2)),
            dma((count, cols, slots)),
            dma((cols,)),
            dma((cols,)),
            dma((2, rows // 2, 2, 2)),
            dma((rows // 2, 2, 2)),
            dma((rows // 2, 2, 2)),
            dma((2,)),
            dma((groups, cols, 2)),
            dma((groups, cols, 2)),
            dma((4,)),
            dma((4,)),
            dma((2,)),
        ],
        compiler_params=pltpu.CompilerParams(has_side_effects=True, vmem_limit_bytes=32 * 1024 * 1024),
        name="exchange",
    )(payload)


def finish_kernel(row_count, marks_ref, tiles_ref, panel_ref, low0_ref, inv0_ref, low1_ref, inv1_ref,
                  out_ref, inv_ref, under_ref, cross_h, cross_l, high_ref, rest_ref, new_ref, new_sem):
    groups, col_count, rows, slots, height, tile = panel_ref.shape
    groups -= 1
    tile_rows, tile_cols = tiles_ref.shape[:2]
    count = 2 * PT
    width = PT * tile
    size = rows * tile
    skip = tile_rows - rows
    first_col = count // col_count
    row = lax.axis_index("row")
    col = lax.axis_index("col")
    span = span_of(tile)

    def write(a, c):
        return pltpu.make_async_copy(new_ref.at[a, c], out_ref.at[a, c], new_sem.at[a, c])

    for a in range(tile_rows):
        for c in range(first_col, tile_cols):
            if a < c // groups or a < skip:
                new_ref[a, c] = jnp.zeros((tile, tile), jnp.float32)
                write(a, c).start()

    def stacked(value):
        high, rest = split(value)
        return jnp.concatenate([high, high, rest], axis=1)

    def dot_stacked(value, weights):
        high, rest = split(value)
        return dot_bf16(jnp.concatenate([high, rest, high], axis=1), weights)

    for k in range(PT // 2):
        inv_ref[k] = stacked(inv0_ref[k])
        inv_ref[PT // 2 + k] = stacked(inv1_ref[k])
    for k, ref in enumerate((low0_ref, low1_ref)):
        for n in range(1, PT // 2):
            under_ref[k, n - 1] = stacked(ref[span(2 * n, 2 * n + 2), span(0, 2)])
    cross_h[...], cross_l[...] = split(low0_ref[span(PT, count), :])

    def solve(group, carry):
        def column(t):
            return panel_ref[group, t % col_count, :, t // col_count, :tile, :].reshape(size, tile)

        def mark(t):
            value = panel_ref[group, t % col_count, :, t // col_count, tile : tile + 1, :]
            return jnp.broadcast_to(value, (rows, tile, tile)).reshape(size, tile)

        def keep(at, value):
            high_ref[group, :, at], rest_ref[group, :, at] = split(value)

        for p in range(2):
            done = None
            for n in range(PT // 2):
                t = p * PT + 2 * n
                value = jnp.concatenate([column(t), column(t + 1)], axis=1)
                if p:
                    high, rest = high_ref[group, :, :width], rest_ref[group, :, :width]
                    at = span(2 * n, 2 * n + 2)
                    coarse = dot_bf16(high, cross_h[at, :])
                    more = dot_bf16(high, cross_l[at, :]) + dot_bf16(rest, cross_h[at, :])
                    marks = jnp.concatenate([mark(t), mark(t + 1)], axis=1)
                    value = value - (coarse + jnp.where(marks > 0.5, 0.0, more))
                if n:
                    value = value - dot_stacked(done, under_ref[p, n - 1])
                done = dot_stacked(value, inv_ref[p * (PT // 2) + n])
                keep(span(t, t + 2), done)
        return carry

    lax.fori_loop(0, 1 + groups, solve, 0)

    def rounded(value):
        return value.astype(jnp.bfloat16).astype(jnp.float32)

    def panel_tile(a, c):
        base = pl.multiple_of((c * col_count + col) * tile, tile)
        is_bf16 = marks_ref[a, c] == 1
        if a >= skip:
            at = slice((a - skip) * tile, (a - skip + 1) * tile)
            rest = rest_ref[0, at, pl.ds(base, tile)].astype(jnp.float32)
            new_ref[a, c] = high_ref[0, at, pl.ds(base, tile)].astype(jnp.float32) + jnp.where(is_bf16, 0.0, rest)
        if a * row_count < count:
            @pl.when(row < count)
            def _():
                place = pl.multiple_of(jnp.minimum(row, count - 1) * tile, tile)
                inner = c * col_count + col

                @pl.when(inner < PT)
                def _():
                    value = low0_ref[pl.ds(place, tile), pl.ds(pl.multiple_of(jnp.minimum(inner, PT - 1) * tile, tile), tile)]
                    new_ref[a, c] = jnp.where(is_bf16, rounded(value), value)

                @pl.when((inner >= PT) & (row >= PT))
                def _():
                    lower = pl.multiple_of(jnp.clip(row - PT, 0, PT - 1) * tile, tile)
                    across = pl.multiple_of(jnp.clip(inner - PT, 0, PT - 1) * tile, tile)
                    value = low1_ref[pl.ds(lower, tile), pl.ds(across, tile)]
                    new_ref[a, c] = jnp.where(is_bf16, rounded(value), value)

                @pl.when(row < inner)
                def _():
                    new_ref[a, c] = jnp.zeros((tile, tile), jnp.float32)

    for a in range(tile_rows):
        for c in range(tile_cols):
            if c < first_col:
                panel_tile(a, c)
                write(a, c).start()
    for b in range(skip, tile_rows):
        at = slice((b - skip) * tile, (b - skip + 1) * tile)
        lower = slice((b - skip) * tile, size)
        high = jnp.concatenate([high_ref[1 + g, at, :] for g in range(groups)], axis=0)
        rest = jnp.concatenate([rest_ref[1 + g, at, :] for g in range(groups)], axis=0)
        coarse = dot_bf16(high_ref[0, lower, :], high)
        more = dot_bf16(high_ref[0, lower, :], rest) + dot_bf16(rest_ref[0, lower, :], high)
        for a in range(b, tile_rows):
            for g in range(groups):
                c = b * groups + g
                if c < first_col:
                    continue
                here = (slice((a - b) * tile, (a - b + 1) * tile), span(g))
                is_bf16 = marks_ref[a, c] == 1
                value = tiles_ref[a, c]
                exact = value - (coarse[here] + more[here])
                value = jnp.where(is_bf16, rounded(rounded(value) - coarse[here]), exact)
                new_ref[a, c] = jnp.where(a * row_count + row >= c * col_count + col, value, 0.0)
                write(a, c).start()
    for a in range(tile_rows):
        for c in range(tile_cols):
            write(a, c).wait()


def finish(marks, tiles, panels, factors, row_count):
    low0, inv0, low1, inv1 = factors
    tile_rows, tile_cols, tile, _ = tiles.shape
    groups, col_count, rows, slots, height, _ = panels.shape
    groups -= 1
    count = 2 * PT
    size = rows * tile
    hbm = pl.BlockSpec(memory_space=pltpu.HBM)
    vmem = pl.BlockSpec(memory_space=pltpu.VMEM)
    dma = pltpu.SemaphoreType.DMA
    bf16 = lambda *shape: pltpu.VMEM(shape, jnp.bfloat16)
    f32 = lambda *shape: pltpu.VMEM(shape, jnp.float32)
    held = 2 * tiles.size + panels.size + low0.size + inv0.size + low1.size + inv1.size
    held += (1 + groups) * size * count * tile + 2 * PT * tile * PT * tile
    return pl.pallas_call(
        lambda *refs: finish_kernel(row_count, *refs),
        out_shape=jax.ShapeDtypeStruct(tiles.shape, jnp.float32),
        in_specs=[pl.BlockSpec(memory_space=pltpu.SMEM)] + [vmem] * 6,
        out_specs=hbm,
        scratch_shapes=[
            bf16(PT, 2 * tile, 6 * tile),
            bf16(2, PT // 2 - 1, 2 * tile, 6 * tile),
            bf16(PT * tile, PT * tile),
            bf16(PT * tile, PT * tile),
            bf16(1 + groups, size, count * tile),
            bf16(1 + groups, size, count * tile),
            f32(*tiles.shape),
            dma((tile_rows, tile_cols)),
        ],
        compiler_params=pltpu.CompilerParams(vmem_limit_bytes=4 * held + 12 * 1024 * 1024),
        name="finish",
    )(marks, tiles, panels, low0, inv0, low1, inv1)


def on_device(matrix, flags):
    row_count = lax.axis_size("row")
    col_count = lax.axis_size("col")
    tile_rows = matrix.shape[0]
    tile_cols = matrix.shape[2]
    tile = matrix.shape[4]
    slots = 2 * PT // col_count
    tiles = matrix.reshape(tile_rows, tile_cols, tile, tile)
    marks = flags.reshape(tile_rows, tile_cols)

    head = tiles[:, :slots]
    head_marks = (marks[:, :slots] == 1)[:, :, None, None]
    stored = jnp.where(head_marks, lax.reduce_precision(head, 8, 7), head)
    tags = jnp.broadcast_to(head_marks.astype(jnp.float32), (tile_rows, slots, 8, tile))
    payload = jnp.concatenate([stored, tags], axis=2)

    panels, _, *factors = exchange(payload, row_count, col_count)
    out = finish(marks, tiles, panels, factors, row_count)
    return out.reshape(matrix.shape)


def solution(mesh):
    return jax.shard_map(
        on_device,
        mesh=mesh,
        in_specs=(P(None, "row", None, "col", None, None), P(None, "row", None, "col")),
        out_specs=P(None, "row", None, "col", None, None),
        check_vma=False,
    )
```
